32 devices in a mesh: unit: 2 (over core), zero: 4 (over z), model: 4 (over y, x).
Axes of the slice: x: 2, y: 2, z: 4, core: 2. Of those that a mesh axis runs over, the one named last changes fastest.
Arguments:
- first_query: float32 [16384, 8192], P(('unit', 'zero'), 'model'), parts along dimension 0, may hold values from -0.09375 to 0.09375
- second_query: float32 [16384, 8192], P(('unit', 'zero'), 'model'), parts along dimension 0, may hold values from -0.0625 to 0.0625
- first_key: float32 [16384, 1024], P(('unit', 'zero'), 'model'), parts along dimension 0, may hold values from -0.09375 to 0.09375
- second_key: float32 [16384, 1024], P(('unit', 'zero'), 'model'), parts along dimension 0, may hold values from -0.0625 to 0.0625
- first_value: float32 [16384, 1024], P(('unit', 'zero'), 'model'), parts along dimension 0, may hold values from -0.09375 to 0.09375
- second_value: float32 [16384, 1024], P(('unit', 'zero'), 'model'), parts along dimension 0, may hold values from -0.0625 to 0.0625
- mix_share: float32 [16384], P(('unit', 'zero')), parts along dimension 0, may hold values from 0.2 to 0.8
- norm_train: float32 [16384], P(('unit', 'zero', 'model')), parts along dimension 0, may hold values from 0.25 to 1.75
- norm_step: float32 [16384], P(('unit', 'zero', 'model')), parts along dimension 0, may hold values from -0.3 to 0.3
Outputs:
- serve_query: bfloat16 [16384, 8192], P('unit', 'model'), parts along dimension 0
- serve_key: bfloat16 [16384, 1024], P('unit', 'model'), parts along dimension 0
- serve_value: bfloat16 [16384, 1024], P('unit', 'model'), parts along dimension 0
- factor_query: float32 [16384], P(('unit', 'model')), parts along dimension 0
- factor_key: float32 [2048], P(('unit', 'model')), parts along dimension 0
- factor_value: float32 [2048], P(('unit', 'model')), parts along dimension 0
- serve_norm: bfloat16 [16384], P('unit'), parts along dimension 0
The draws below stay inside these ranges and needn't reach their ends.
There are 2 independent parts, one for each index of `unit`. The reference program is written for one: setup_inputs(seed, part) draws one part's arguments, and reference() takes and returns one part's arrays. A program takes and returns all parts, laid end to end along the dimension named above; each array names one. Nothing has to cross between parts.
All inputs are finite; a program needn't handle non-finite values.
Results may differ from the reference program's by a relative error of at most 0.0004.
Values may be sent and summed in bfloat16 or wider, within the bound.
A program may use at most 192 MiB of HBM per device.

```python
import jax
import jax.numpy as jnp
from jax import lax

D_MODEL = 8192
Q_DIM = 8192
KV_DIM = 1024


def with_spikes(values, rng, source, target, shards_of, factor):
    owner, partner = [(jnp.arange(values.shape[dim]) // (values.shape[dim] // shards_of)).reshape([-1 if axis == dim else 1 for axis in range(values.ndim)]) for dim in (source, target)]
    chosen = jax.random.permutation(rng, shards_of)[partner]
    strong = (owner == chosen) | (owner == (partner + shards_of // 2) % shards_of)
    return jnp.where(strong, factor * values, values)


def level_of(rng, shape, cuts, smallest, high):
    def one(axis_at, blocks):
        draws = jax.random.uniform(jax.random.fold_in(jax.random.fold_in(rng, 6), axis_at), (blocks,), jnp.float32, smallest / len(cuts), high / len(cuts))
        return jnp.repeat(jnp.exp(draws), shape[axis_at] // blocks).reshape((-1,) + (1,) * (len(shape) - axis_at - 1))

    loudness = one(*cuts[0])
    for cut in cuts[1:]:
        loudness = loudness * one(*cut)
    return loudness


def normal_values(stream_key, extent, deviation, reach, cuts=(), dtype=jnp.bfloat16):
    entries = deviation * jax.random.normal(stream_key, extent, jnp.float32)
    if cuts:
        entries = entries * level_of(stream_key, extent, cuts, -0.22, 0.18)
    return jnp.clip(entries, -reach, reach).astype(dtype)


def noise_with(own_key, extent, deviation, most, cuts, heavy, held_as=jnp.bfloat16):
    values = deviation * jax.random.normal(own_key, extent, jnp.float32)
    if cuts:
        values = values * level_of(own_key, extent, cuts, -0.22, 0.18)
    return jnp.clip(with_spikes(values, jax.random.fold_in(own_key, 3), *heavy), -most, most).astype(held_as)


def setup_inputs(seed: int = 0, part: int = 0) -> dict:
    key_list = jax.random.split(jax.random.key(seed), 10)
    own_keys = jax.random.split(jax.random.fold_in(key_list[9], part), 10)
    return {
        "first_query": noise_with(own_keys[0], (D_MODEL, Q_DIM), D_MODEL ** -0.5, 0.09375, ((0, 4), (1, 4)), (0, 1, 4, 2.0), jnp.float32),
        "second_query": normal_values(own_keys[1], (D_MODEL, Q_DIM), D_MODEL ** -0.5, 0.0625, ((0, 4), (1, 4)), jnp.float32),
        "first_key": noise_with(own_keys[2], (D_MODEL, KV_DIM), D_MODEL ** -0.5, 0.09375, ((0, 4), (1, 4)), (0, 1, 4, 2.0), jnp.float32),
        "second_key": normal_values(own_keys[3], (D_MODEL, KV_DIM), D_MODEL ** -0.5, 0.0625, ((0, 4), (1, 4)), jnp.float32),
        "first_value": noise_with(own_keys[4], (D_MODEL, KV_DIM), D_MODEL ** -0.5, 0.09375, ((0, 4), (1, 4)), (0, 1, 4, 2.0), jnp.float32),
        "second_value": normal_values(own_keys[5], (D_MODEL, KV_DIM), D_MODEL ** -0.5, 0.0625, ((0, 4), (1, 4)), jnp.float32),
        "mix_share": jnp.clip(0.2 + 0.6 * jax.random.uniform(own_keys[6], (D_MODEL,), jnp.float32) ** level_of(own_keys[6], (D_MODEL,), ((0, 4),), -0.2, 0.2), 0.2, 0.8),
        "norm_train": jnp.clip(1.0 + 0.15 * jax.random.normal(own_keys[7], (D_MODEL,), jnp.float32), 0.25, 1.75),
        "norm_step": jnp.clip(jax.random.uniform(own_keys[8], (D_MODEL,), jnp.float32, -0.3, 0.3) * level_of(own_keys[8], (D_MODEL,), ((0, 16),), -0.4, 0.0), -0.3, 0.3),
    }


def reference(first_query, second_query, first_key, second_key, first_value, second_value, mix_share, norm_train, norm_step):
    fresh_query = mix_share[:, None] * first_query + (1.0 - mix_share[:, None]) * second_query
    fresh_key = mix_share[:, None] * first_key + (1.0 - mix_share[:, None]) * second_key
    fresh_value = mix_share[:, None] * first_value + (1.0 - mix_share[:, None]) * second_value
    factor_query = jnp.sqrt(lax.optimization_barrier(jnp.sum(fresh_query * fresh_query, axis=0)))
    serve_query = (fresh_query / factor_query).astype(jnp.bfloat16)
    factor_key = jnp.sqrt(lax.optimization_barrier(jnp.sum(fresh_key * fresh_key, axis=0)))
    serve_key = (fresh_key / factor_key).astype(jnp.bfloat16)
    factor_value = jnp.sqrt(lax.optimization_barrier(jnp.sum(fresh_value * fresh_value, axis=0)))
    serve_value = (fresh_value / factor_value).astype(jnp.bfloat16)
    serve_norm = (norm_train + norm_step).astype(jnp.bfloat16)
    return (serve_query, serve_key, serve_value, factor_query, factor_key, factor_value, serve_norm)
```

```python
import functools

import jax
import jax.numpy as jnp
from jax import lax
from jax.experimental import pallas as pl
from jax.experimental.pallas import tpu as pltpu
from jax.sharding import PartitionSpec as P


MESH = pl.DeviceIdType.MESH
LANES = 128
READS = 4
SHARES = (4, 4, 4, 3, 1)


def total_of(held, n_zero):
    total = held[0]
    for k in range(1, n_zero):
        total = total + held[k]
    return total


def lead_kernel(
    n_zero,
    first_key,
    second_key,
    first_value,
    second_value,
    share_ref,
    train_ref,
    step_ref,
    block_ref,
    key_total,
    value_total,
    gain_ref,
    key_a,
    key_b,
    value_a,
    value_b,
    wide,
    narrow,
    norm,
    key_held,
    value_held,
    key_part,
    value_part,
    read_sem,
    write_sem,
    sent,
    got,
    own,
):
    z = lax.axis_index("zero")
    rows, width = key_a.shape
    step = rows // READS
    barrier = pltpu.get_barrier_semaphore()
    peers = [lax.rem(z + k, n_zero) for k in range(1, n_zero)]
    for peer in peers:
        pl.semaphore_signal(barrier, inc=1, device_id={"zero": peer}, device_id_type=MESH)

    reads = []
    for which, (source, target) in enumerate(
        ((first_key, key_a), (second_key, key_b), (first_value, value_a), (second_value, value_b))
    ):
        reads.append([])
        for k in range(READS):
            part = pl.ds(k * step, step)
            reads[-1].append(pltpu.make_async_copy(source.at[part], target.at[part], read_sem.at[which, k]))
    for pair in (reads[:2], reads[2:]):
        for k in range(READS):
            for group in pair:
                group[k].start()

    norm[...] = (train_ref[...] + step_ref[...]).astype(norm.dtype)
    lanes = min(LANES, width)
    for k in range(rows // LANES):
        line = jnp.broadcast_to(share_ref[k : k + 1, :], (LANES, LANES))
        wide[k * LANES : (k + 1) * LANES, :] = jnp.transpose(line)

    def sums(first, second, groups, target):
        size = min(LANES, step)
        sums_of = [jnp.zeros((8, min(lanes, width - low)), jnp.float32) for low in range(0, width, lanes)]
        for k in range(READS):
            for group in groups:
                group[k].wait()
            for low in range(k * step, (k + 1) * step, size):
                for c in range(len(sums_of)):
                    columns = pl.ds(c * lanes, sums_of[c].shape[1])
                    here = pl.ds(low, size)
                    share = wide[here, : sums_of[c].shape[1]]
                    fresh = share * first[here, columns] + (1.0 - share) * second[here, columns]
                    first[here, columns] = fresh
                    square = fresh * fresh
                    sums_of[c] = sums_of[c] + jnp.sum(square.reshape(size // 8, 8, square.shape[1]), axis=0)
        for c, value in enumerate(sums_of):
            target[:, c * lanes : c * lanes + value.shape[1]] = jnp.sum(value, axis=0, keepdims=True)

    def exchange(index, source, target):
        copies = []
        for k, peer in enumerate(peers, 1):
            copies.append(
                pltpu.make_async_remote_copy(
                    src_ref=source,
                    dst_ref=target.at[z],
                    send_sem=sent.at[index, k],
                    recv_sem=got.at[index, k],
                    device_id={"zero": peer},
                    device_id_type=MESH,
                )
            )
        for copy in copies:
            copy.start()
        return copies

    sums(key_a, key_b, reads[:2], key_part)
    pl.semaphore_wait(barrier, n_zero - 1)
    key_copies = exchange(0, key_part, key_held)
    key_held[z] = key_part[...]
    sums(value_a, value_b, reads[2:], value_part)
    value_held[z] = value_part[...]
    mine = pltpu.make_async_copy(norm, gain_ref.at[z], own)
    mine.start()
    value_copies = exchange(1, value_part, value_held)
    norm_copies = exchange(2, norm, gain_ref)

    for copy in key_copies:
        copy.wait()
    total = total_of(key_held, n_zero)
    key_total[...] = total
    scale = 1.0 / jnp.sqrt(total)
    writes = []
    for k in range(READS):
        part = pl.ds(k * step, step)
        narrow[part, :] = (key_a[part, :] * scale).astype(narrow.dtype)
        writes.append(pltpu.make_async_copy(narrow.at[part], block_ref.at[part], write_sem.at[k]))
        writes[-1].start()
    for copy in value_copies:
        copy.wait()
    value_total[...] = total_of(value_held, n_zero)
    for copy in norm_copies + writes + [mine]:
        copy.wait()


def lead(n_zero, first_key, second_key, first_value, second_value, share, train, step):
    vmem = pl.BlockSpec(memory_space=pltpu.VMEM)
    hbm = pl.BlockSpec(memory_space=pl.ANY)
    shape = first_key.shape
    rows, width = shape
    part = (1, width)
    return pl.pallas_call(
        functools.partial(lead_kernel, n_zero),
        out_shape=(
            jax.ShapeDtypeStruct(shape, jnp.bfloat16),
            jax.ShapeDtypeStruct(part, jnp.float32),
            jax.ShapeDtypeStruct(part, jnp.float32),
            jax.ShapeDtypeStruct((n_zero,) + train.shape, jnp.bfloat16),
        ),
        in_specs=[hbm] * 4 + [vmem] * 3,
        out_specs=(hbm, vmem, vmem, vmem),
        scratch_shapes=[pltpu.VMEM(shape, jnp.float32)] * 4
        + [
            pltpu.VMEM((rows, LANES), jnp.float32),
            pltpu.VMEM(shape, jnp.bfloat16),
            pltpu.VMEM(train.shape, jnp.bfloat16),
            pltpu.VMEM((n_zero,) + part, jnp.float32),
            pltpu.VMEM((n_zero,) + part, jnp.float32),
            pltpu.VMEM(part, jnp.float32),
            pltpu.VMEM(part, jnp.float32),
            pltpu.SemaphoreType.DMA((4, READS)),
            pltpu.SemaphoreType.DMA((READS,)),
            pltpu.SemaphoreType.DMA((3, n_zero)),
            pltpu.SemaphoreType.DMA((3, n_zero)),
            pltpu.SemaphoreType.DMA,
        ],
        compiler_params=pltpu.CompilerParams(collective_id=0, has_side_effects=True),
        name="lead",
    )(first_key, second_key, first_value, second_value, share, train, step)


def spread_kernel(n_model, part_ref, all_ref, sent, got, own):
    m = lax.axis_index("model")
    barrier = pltpu.get_barrier_semaphore()
    peers = [lax.rem(m + k, n_model) for k in range(1, n_model)]
    for peer in peers:
        pl.semaphore_signal(barrier, inc=1, device_id={"model": peer}, device_id_type=MESH)
    mine = pltpu.make_async_copy(part_ref, all_ref.at[m], own)
    mine.start()
    pl.semaphore_wait(barrier, n_model - 1)
    copies = []
    for k, peer in enumerate(peers, 1):
        copies.append(
            pltpu.make_async_remote_copy(
                src_ref=part_ref,
                dst_ref=all_ref.at[m],
                send_sem=sent.at[k],
                recv_sem=got.at[k],
                device_id={"model": peer},
                device_id_type=MESH,
            )
        )
    for copy in copies:
        copy.start()
    for copy in copies + [mine]:
        copy.wait()


def spread(n_model, part):
    vmem = pl.BlockSpec(memory_space=pltpu.VMEM)
    return pl.pallas_call(
        functools.partial(spread_kernel, n_model),
        out_shape=jax.ShapeDtypeStruct((n_model,) + part.shape, part.dtype),
        in_specs=[vmem],
        out_specs=vmem,
        scratch_shapes=[
            pltpu.SemaphoreType.DMA((n_model,)),
            pltpu.SemaphoreType.DMA((n_model,)),
            pltpu.SemaphoreType.DMA,
        ],
        compiler_params=pltpu.CompilerParams(collective_id=1, has_side_effects=True),
        name="spread",
    )(part)


def piece_bounds(rows):
    bounds, low = [], 0
    for share in SHARES:
        high = low + rows * share // sum(SHARES)
        bounds.append((low, high))
        low = high
    return bounds


def merge(
    n_zero,
    n_model,
    first_query,
    second_query,
    first_key,
    second_key,
    first_value,
    second_value,
    mix_share,
    norm_train,
    norm_step,
):
    rows = mix_share.shape[0]
    z = lax.axis_index("zero")
    up = [[(k, k + 1) for k in range(hop, n_zero - 1)] for hop in range(n_zero - 1)]
    down = [[(k, k - 1) for k in range(1, n_zero - hop)] for hop in range(n_zero - 1)]
    ring = [[(k, (k + shift) % n_zero) for k in range(n_zero)] for shift in range(n_zero)]

    key_block, key_total, value_total, gain = lead(
        n_zero,
        first_key,
        second_key,
        first_value,
        second_value,
        mix_share.reshape(-1, LANES),
        norm_train[None, :],
        norm_step[None, :],
    )
    factors = [None, jnp.sqrt(key_total[0]), jnp.sqrt(value_total[0])]

    def send(block, hop):
        above = lax.ppermute(block[0], "zero", up[hop])
        below = lax.ppermute(block[1], "zero", down[hop])
        return above, below

    key_moved = send((key_block, key_block), 0)
    first_query, second_query, first_value, second_value, share, _ = lax.optimization_barrier(
        (first_query, second_query, first_value, second_value, mix_share, key_block)
    )
    share = share[:, None]
    pairs = ((first_query, second_query), None, (first_value, second_value))

    def fresh_of(which, low, high):
        first, second = pairs[which][0][low:high], pairs[which][1][low:high]
        return share[low:high] * first + (1.0 - share[low:high]) * second

    def narrow(which, low, high, after=None):
        scale = factors[which]
        if after is not None:
            scale, _ = lax.optimization_barrier((scale, after))
        block = (fresh_of(which, low, high) / scale).astype(jnp.bfloat16)
        return lax.optimization_barrier(block)

    value_block = narrow(2, 0, rows)
    fresh = fresh_of(0, 0, rows)
    part = jnp.sum(fresh * fresh, axis=0)
    part, value_block = lax.optimization_barrier((part, value_block))
    parts = [part]
    for shift in range(1, n_zero):
        parts.append(lax.ppermute(part, "zero", ring[shift]))
    stack = jnp.stack(parts)
    total = sum(
        lax.dynamic_index_in_dim(stack, lax.rem(z + n_zero - k, n_zero), 0, keepdims=False)
        for k in range(n_zero)
    )
    factors[0] = jnp.sqrt(total)

    pieces = [(1, 0, rows), (2, 0, rows)]
    pieces += [(0, low, high) for low, high in piece_bounds(rows)]
    blocks = [key_block, value_block]
    for k, piece in enumerate(pieces[2:], 2):
        blocks.append(narrow(*piece, after=blocks[-1]))
    gain, factors[1], _ = lax.optimization_barrier((gain, factors[1], blocks[-1]))
    gain = spread(n_model, gain)

    widths = [first_query.shape[1], first_key.shape[1], first_value.shape[1]]
    serve = [jnp.zeros((n_zero * rows, width), jnp.bfloat16) for width in widths]

    def place(piece, block, owner):
        which, low, _ = piece
        serve[which] = lax.dynamic_update_slice(serve[which], block, (owner * rows + low, jnp.zeros_like(owner)))

    for piece, block in zip(pieces, blocks):
        place(piece, block, z)
    above, below = {}, {}
    flying = [(block, block) for block in blocks]
    for hop in range(n_zero - 1):
        for k, piece in enumerate(pieces):
            flying[k] = key_moved if (hop, k) == (0, 0) else send(flying[k], hop)
            above[hop + 1, k], below[hop + 1, k] = flying[k]
        for k, piece in enumerate(pieces):
            for away in range(1, n_zero):
                if max(away, n_zero - away) == hop + 1:
                    block = jnp.where(z + away < n_zero, below[away, k], above[n_zero - away, k])
                    place(piece, block, lax.rem(z + away, n_zero))
    gain = gain.reshape(n_model, n_zero, -1).transpose(1, 0, 2)
    return (*serve, *factors, gain.reshape(-1))


def solution(mesh):
    in_specs = (
        P(("unit", "zero"), "model"),
        P(("unit", "zero"), "model"),
        P(("unit", "zero"), "model"),
        P(("unit", "zero"), "model"),
        P(("unit", "zero"), "model"),
        P(("unit", "zero"), "model"),
        P(("unit", "zero")),
        P(("unit", "zero", "model")),
        P(("unit", "zero", "model")),
    )
    out_specs = (
        P("unit", "model"),
        P("unit", "model"),
        P("unit", "model"),
        P(("unit", "model")),
        P(("unit", "model")),
        P(("unit", "model")),
        P("unit"),
    )
    return jax.shard_map(
        functools.partial(merge, mesh.shape["zero"], mesh.shape["model"]),
        mesh=mesh,
        in_specs=in_specs,
        out_specs=out_specs,
        check_vma=False,
    )
```

```python
import functools

import jax
import jax.numpy as jnp
from jax import lax
from jax.experimental import pallas as pl
from jax.experimental.pallas import tpu as pltpu
from jax.sharding import PartitionSpec as P


MESH = pl.DeviceIdType.MESH
LANES = 128
READS = 4
SHARES = (4, 4, 4, 3, 1)


def total_of(held, n_zero):
    total = held[0]
    for k in range(1, n_zero):
        total = total + held[k]
    return total


def lead_kernel(
    n_zero,
    first_key,
    second_key,
    first_value,
    second_value,
    share_ref,
    train_ref,
    step_ref,
    block_ref,
    key_total,
    value_total,
    gain_ref,
    key_a,
    key_b,
    value_a,
    value_b,
    wide,
    narrow,
    norm,
    key_held,
    value_held,
    key_part,
    value_part,
    read_sem,
    write_sem,
    sent,
    got,
    own,
):
    z = lax.axis_index("zero")
    rows, width = key_a.shape
    step = rows // READS
    barrier = pltpu.get_barrier_semaphore()
    peers = [lax.rem(z + k, n_zero) for k in range(1, n_zero)]
    for peer in peers:
        pl.semaphore_signal(barrier, inc=1, device_id={"zero": peer}, device_id_type=MESH)

    reads = []
    for which, (source, target) in enumerate(
        ((first_key, key_a), (second_key, key_b), (first_value, value_a), (second_value, value_b))
    ):
        reads.append([])
        for k in range(READS):
            part = pl.ds(k * step, step)
            reads[-1].append(pltpu.make_async_copy(source.at[part], target.at[part], read_sem.at[which, k]))
    for pair in (reads[:2], reads[2:]):
        for k in range(READS):
            for group in pair:
                group[k].start()

    norm[...] = (train_ref[...] + step_ref[...]).astype(norm.dtype)
    lanes = min(LANES, width)
    for k in range(rows // LANES):
        line = jnp.broadcast_to(share_ref[k : k + 1, :], (LANES, LANES))
        wide[k * LANES : (k + 1) * LANES, :] = jnp.transpose(line)

    def sums(first, second, groups, target):
        size = min(LANES, step)
        sums_of = [jnp.zeros((8, min(lanes, width - low)), jnp.float32) for low in range(0, width, lanes)]
        for k in range(READS):
            for group in groups:
                group[k].wait()
            for low in range(k * step, (k + 1) * step, size):
                for c in range(len(sums_of)):
                    columns = pl.ds(c * lanes, sums_of[c].shape[1])
                    here = pl.ds(low, size)
                    share = wide[here, : sums_of[c].shape[1]]
                    fresh = share * first[here, columns] + (1.0 - share) * second[here, columns]
                    first[here, columns] = fresh
                    square = fresh * fresh
                    sums_of[c] = sums_of[c] + jnp.sum(square.reshape(size // 8, 8, square.shape[1]), axis=0)
        for c, value in enumerate(sums_of):
            target[:, c * lanes : c * lanes + value.shape[1]] = jnp.sum(value, axis=0, keepdims=True)

    def exchange(index, source, target):
        copies = []
        for k, peer in enumerate(peers, 1):
            copies.append(
                pltpu.make_async_remote_copy(
                    src_ref=source,
                    dst_ref=target.at[z],
                    send_sem=sent.at[index, k],
                    recv_sem=got.at[index, k],
                    device_id={"zero": peer},
                    device_id_type=MESH,
                )
            )
        for copy in copies:
            copy.start()
        return copies

    sums(key_a, key_b, reads[:2], key_part)
    pl.semaphore_wait(barrier, n_zero - 1)
    key_copies = exchange(0, key_part, key_held)
    key_held[z] = key_part[...]
    sums(value_a, value_b, reads[2:], value_part)
    value_held[z] = value_part[...]
    mine = pltpu.make_async_copy(norm, gain_ref.at[z], own)
    mine.start()
    value_copies = exchange(1, value_part, value_held)
    norm_copies = exchange(2, norm, gain_ref)

    for copy in key_copies:
        copy.wait()
    total = total_of(key_held, n_zero)
    key_total[...] = total
    scale = 1.0 / jnp.sqrt(total)
    writes = []
    for k in range(READS):
        part = pl.ds(k * step, step)
        narrow[part, :] = (key_a[part, :] * scale).astype(narrow.dtype)
        writes.append(pltpu.make_async_copy(narrow.at[part], block_ref.at[part], write_sem.at[k]))
        writes[-1].start()
    for copy in value_copies:
        copy.wait()
    value_total[...] = total_of(value_held, n_zero)
    for copy in norm_copies + writes + [mine]:
        copy.wait()


def lead(n_zero, first_key, second_key, first_value, second_value, share, train, step):
    vmem = pl.BlockSpec(memory_space=pltpu.VMEM)
    hbm = pl.BlockSpec(memory_space=pl.ANY)
    shape = first_key.shape
    rows, width = shape
    part = (1, width)
    return pl.pallas_call(
        functools.partial(lead_kernel, n_zero),
        out_shape=(
            jax.ShapeDtypeStruct(shape, jnp.bfloat16),
            jax.ShapeDtypeStruct(part, jnp.float32),
            jax.ShapeDtypeStruct(part, jnp.float32),
            jax.ShapeDtypeStruct((n_zero,) + train.shape, jnp.bfloat16),
        ),
        in_specs=[hbm] * 4 + [vmem] * 3,
        out_specs=(hbm, vmem, vmem, vmem),
        scratch_shapes=[pltpu.VMEM(shape, jnp.float32)] * 4
        + [
            pltpu.VMEM((rows, LANES), jnp.float32),
            pltpu.VMEM(shape, jnp.bfloat16),
            pltpu.VMEM(train.shape, jnp.bfloat16),
            pltpu.VMEM((n_zero,) + part, jnp.float32),
            pltpu.VMEM((n_zero,) + part, jnp.float32),
            pltpu.VMEM(part, jnp.float32),
            pltpu.VMEM(part, jnp.float32),
            pltpu.SemaphoreType.DMA((4, READS)),
            pltpu.SemaphoreType.DMA((READS,)),
            pltpu.SemaphoreType.DMA((3, n_zero)),
            pltpu.SemaphoreType.DMA((3, n_zero)),
            pltpu.SemaphoreType.DMA,
        ],
        compiler_params=pltpu.CompilerParams(collective_id=0, has_side_effects=True),
        name="lead",
    )(first_key, second_key, first_value, second_value, share, train, step)


def spread_kernel(n_model, part_ref, all_ref, sent, got, own):
    m = lax.axis_index("model")
    barrier = pltpu.get_barrier_semaphore()
    peers = [lax.rem(m + k, n_model) for k in range(1, n_model)]
    for peer in peers:
        pl.semaphore_signal(barrier, inc=1, device_id={"model": peer}, device_id_type=MESH)
    mine = pltpu.make_async_copy(part_ref, all_ref.at[m], own)
    mine.start()
    pl.semaphore_wait(barrier, n_model - 1)
    copies = []
    for k, peer in enumerate(peers, 1):
        copies.append(
            pltpu.make_async_remote_copy(
                src_ref=part_ref,
                dst_ref=all_ref.at[m],
                send_sem=sent.at[k],
                recv_sem=got.at[k],
                device_id={"model": peer},
                device_id_type=MESH,
            )
        )
    for copy in copies:
        copy.start()
    for copy in copies + [mine]:
        copy.wait()


def spread(n_model, part):
    vmem = pl.BlockSpec(memory_space=pltpu.VMEM)
    return pl.pallas_call(
        functools.partial(spread_kernel, n_model),
        out_shape=jax.ShapeDtypeStruct((n_model,) + part.shape, part.dtype),
        in_specs=[vmem],
        out_specs=vmem,
        scratch_shapes=[
            pltpu.SemaphoreType.DMA((n_model,)),
            pltpu.SemaphoreType.DMA((n_model,)),
            pltpu.SemaphoreType.DMA,
        ],
        compiler_params=pltpu.CompilerParams(collective_id=1, has_side_effects=True),
        name="spread",
    )(part)


def piece_bounds(rows):
    bounds, low = [], 0
    for share in SHARES:
        high = low + rows * share // sum(SHARES)
        bounds.append((low, high))
        low = high
    return bounds


def merge(
    n_zero,
    n_model,
    first_query,
    second_query,
    first_key,
    second_key,
    first_value,
    second_value,
    mix_share,
    norm_train,
    norm_step,
):
    rows = mix_share.shape[0]
    z = lax.axis_index("zero")
    ring = [[(k, (k + shift) % n_zero) for k in range(n_zero)] for shift in range(n_zero)]

    key_block, key_total, value_total, gain = lead(
        n_zero,
        first_key,
        second_key,
        first_value,
        second_value,
        mix_share.reshape(-1, LANES),
        norm_train[None, :],
        norm_step[None, :],
    )
    factors = [None, jnp.sqrt(key_total[0]), jnp.sqrt(value_total[0])]

    def send(block):
        return lax.ppermute(block, "zero", ring[1])

    key_moved = send(key_block)
    first_query, second_query, first_value, second_value, share, _ = lax.optimization_barrier(
        (first_query, second_query, first_value, second_value, mix_share, key_block)
    )
    share = share[:, None]
    pairs = ((first_query, second_query), None, (first_value, second_value))

    def fresh_of(which, low, high):
        first, second = pairs[which][0][low:high], pairs[which][1][low:high]
        return share[low:high] * first + (1.0 - share[low:high]) * second

    def narrow(which, low, high, after=None):
        scale = factors[which]
        if after is not None:
            scale, _ = lax.optimization_barrier((scale, after))
        block = (fresh_of(which, low, high) / scale).astype(jnp.bfloat16)
        return lax.optimization_barrier(block)

    value_block = narrow(2, 0, rows)
    fresh = fresh_of(0, 0, rows)
    part = jnp.sum(fresh * fresh, axis=0)
    part, value_block = lax.optimization_barrier((part, value_block))
    parts = [part]
    for shift in range(1, n_zero):
        parts.append(lax.ppermute(part, "zero", ring[shift]))
    stack = jnp.stack(parts)
    total = sum(
        lax.dynamic_index_in_dim(stack, lax.rem(z + n_zero - k, n_zero), 0, keepdims=False)
        for k in range(n_zero)
    )
    factors[0] = jnp.sqrt(total)

    pieces = [(1, 0, rows), (2, 0, rows)]
    pieces += [(0, low, high) for low, high in piece_bounds(rows)]
    blocks = [key_block, value_block]
    for k, piece in enumerate(pieces[2:], 2):
        blocks.append(narrow(*piece, after=blocks[-1]))
    gain, factors[1], _ = lax.optimization_barrier((gain, factors[1], blocks[-1]))
    gain = spread(n_model, gain)

    widths = [first_query.shape[1], first_key.shape[1], first_value.shape[1]]
    serve = [jnp.zeros((n_zero * rows, width), jnp.bfloat16) for width in widths]

    for hop in range(n_zero):
        owner = lax.rem(z + n_zero - hop, n_zero)
        moved = []
        for k, ((which, low, _), block) in enumerate(zip(pieces, blocks)):
            if hop < n_zero - 1:
                moved.append(key_moved if (hop, k) == (0, 0) else send(block))
            serve[which] = lax.dynamic_update_slice(
                serve[which], block, (owner * rows + low, jnp.zeros_like(owner))
            )
        blocks = moved
    gain = gain.reshape(n_model, n_zero, -1).transpose(1, 0, 2)
    return (*serve, *factors, gain.reshape(-1))


def solution(mesh):
    in_specs = (
        P(("unit", "zero"), "model"),
        P(("unit", "zero"), "model"),
        P(("unit", "zero"), "model"),
        P(("unit", "zero"), "model"),
        P(("unit", "zero"), "model"),
        P(("unit", "zero"), "model"),
        P(("unit", "zero")),
        P(("unit", "zero", "model")),
        P(("unit", "zero", "model")),
    )
    out_specs = (
        P("unit", "model"),
        P("unit", "model"),
        P("unit", "model"),
        P(("unit", "model")),
        P(("unit", "model")),
        P(("unit", "model")),
        P("unit"),
    )
    return jax.shard_map(
        functools.partial(merge, mesh.shape["zero"], mesh.shape["model"]),
        mesh=mesh,
        in_specs=in_specs,
        out_specs=out_specs,
        check_vma=False,
    )
```

```python
import functools

import jax
import jax.numpy as jnp
from jax import lax
from jax.experimental import pallas as pl
from jax.experimental.pallas import tpu as pltpu
from jax.sharding import PartitionSpec as P

MESH = pl.DeviceIdType.MESH
LANES = 128
GROUP = 32
EARLY = 4
CHUNKS = 16
SPLIT = 16
CUTS = (0, 4, 8, 12, 15, 16)
LATE = 2


def total_of(held, n_zero):
    total = held[0]
    for k in range(1, n_zero):
        total = total + held[k]
    return total


def slabs_of(width):
    return [(low, min(LANES, width - low)) for low in range(0, width, LANES)]


def mix_rows(first, second, wide, low, count, sums):
    group = min(GROUP, count)
    slabs = slabs_of(first.shape[1])

    def step(i, sums):
        here = pl.ds(pl.multiple_of(low + i * group, group), group)
        share = wide[here, :]
        rest = 1.0 - share
        out = []
        for (start, size), total in zip(slabs, sums):
            columns = pl.ds(start, size)
            fresh = share[:, :size] * first[here, columns] + rest[:, :size] * second[here, columns]
            first[here, columns] = fresh
            out.append(total + jnp.sum((fresh * fresh).reshape(group // 8, 8, size), axis=0))
        return tuple(out)

    return lax.fori_loop(0, count // group, step, tuple(sums))


def narrow_rows(fresh, own, scale, low, count):
    group = min(GROUP, count)
    slabs = slabs_of(fresh.shape[1])
    scales = [jnp.broadcast_to(scale[:, start : start + size], (group, size)) for start, size in slabs]

    def step(i, carry):
        here = pl.ds(pl.multiple_of(low + i * group, group), group)
        for (start, size), factor in zip(slabs, scales):
            columns = pl.ds(start, size)
            own[here, columns] = (fresh[here, columns] * factor).astype(own.dtype)
        return carry

    lax.fori_loop(0, count // group, step, 0)


def carry_kernel(n_zero, pieces, *refs):
    inputs, outputs, scratch = refs[:9], refs[9 : 16 + LATE], refs[16 + LATE :]
    sources = (inputs[0:2], inputs[2:4], inputs[4:6])
    share_ref, train_ref, step_ref = inputs[6:]
    serve, totals, gain_ref = outputs[0:3], outputs[3:6], outputs[6]
    late_refs = outputs[7:]
    fresh, second, own = scratch[0:3], scratch[3:6], scratch[6:9]
    wide, norm = scratch[9:11]
    held, part = scratch[11:14], scratch[14:17]
    read_sem, own_sem, late_sem, stat_sent, stat_got, norm_sem, sent, got = scratch[17:]

    z = lax.axis_index("zero")
    rows = fresh[0].shape[0]
    barrier = pltpu.get_barrier_semaphore()
    peers = [lax.rem(z + k, n_zero) for k in range(1, n_zero)]
    for peer in peers:
        pl.semaphore_signal(barrier, inc=1, device_id={"zero": peer}, device_id_type=MESH)

    def read(which, k, chunks):
        step = rows // chunks
        here = pl.ds(k * step, step)
        return [
            pltpu.make_async_copy(source.at[here], target.at[here], read_sem.at[which, side, k])
            for side, (source, target) in enumerate(zip(sources[which], (fresh[which], second[which])))
        ]

    def start(copies):
        for copy in copies:
            copy.start()

    def finish(copies):
        for copy in copies:
            copy.wait()

    for k in range(EARLY):
        start(read(1, k, EARLY))
    norm[...] = (train_ref[...] + step_ref[...]).astype(norm.dtype)
    for k in range(rows // LANES):
        line = jnp.broadcast_to(share_ref[k : k + 1, :], (LANES, LANES))
        wide[k * LANES : (k + 1) * LANES, :] = jnp.transpose(line)

    def sums_start(which):
        return tuple(jnp.zeros((8, size), jnp.float32) for _, size in slabs_of(fresh[which].shape[1]))

    def tally(which, sums, low, high, chunks):
        step = rows // chunks
        for k in range(low, high):
            finish(read(which, k, chunks))
            sums = mix_rows(fresh[which], second[which], wide, k * step, step, sums)
        return sums

    def close(which, sums):
        for (start_at, size), value in zip(slabs_of(fresh[which].shape[1]), sums):
            part[which][:, start_at : start_at + size] = jnp.sum(value, axis=0, keepdims=True)

    def exchange(index, source, target):
        copies = []
        for k, peer in enumerate(peers, 1):
            copies.append(
                pltpu.make_async_remote_copy(
                    src_ref=source,
                    dst_ref=target.at[z],
                    send_sem=stat_sent.at[index, k],
                    recv_sem=stat_got.at[index, k],
                    device_id={"zero": peer},
                    device_id_type=MESH,
                )
            )
        start(copies)
        return copies

    def move(p, hop, way, owner, source=None):
        which, low, count, _ = pieces[p]
        here = pl.ds(pl.multiple_of(owner * rows + low, 8), count)
        target = serve[which].at[here]
        return pltpu.make_async_remote_copy(
            src_ref=target if source is None else source,
            dst_ref=target,
            send_sem=sent.at[way, p],
            recv_sem=got.at[way, hop, p],
            device_id={"zero": lax.rem(z + (1 if way == 0 else n_zero - 1), n_zero)},
            device_id_type=MESH,
        )

    ranks = (z, n_zero - 1 - z)

    def sends(p, hop, way):
        rank = ranks[way]
        yes = jnp.logical_and(rank < n_zero - 1, rank >= hop)
        if pieces[p][3]:
            yes = jnp.logical_and(yes, jnp.logical_not(jnp.logical_and(hop == 0, rank == n_zero - 2)))
        return yes

    def arrives(p, hop, way):
        rank = ranks[way]
        yes = rank >= hop + 1
        if pieces[p][3]:
            yes = jnp.logical_and(yes, jnp.logical_not(jnp.logical_and(hop == 0, rank == n_zero - 1)))
        return yes

    def own_copies(p):
        which, low, count, late = pieces[p]
        source = own[which].at[pl.ds(low, count)]
        here = pl.ds(pl.multiple_of(z * rows + low, 8), count)
        copies = [pltpu.make_async_copy(source, serve[which].at[here], own_sem.at[p])]
        if late:
            copies.append(pltpu.make_async_copy(source, late_refs[late - 1], late_sem.at[late - 1]))
        return copies

    def first_move(p, way):
        which, low, count, _ = pieces[p]
        return move(p, 0, way, z, own[which].at[pl.ds(low, count)])

    def launch(p):
        for way in (0, 1):

            @pl.when(sends(p, 0, way))
            def _():
                first_move(p, way).start()

        start(own_copies(p))

    def settle(which, copies):
        finish(copies)
        total = total_of(held[which], n_zero)
        totals[which][...] = total
        return 1.0 / jnp.sqrt(total)

    sums = tally(1, sums_start(1), 0, EARLY // 2, EARLY)
    for k in range(EARLY):
        start(read(2, k, EARLY))
    sums = tally(1, sums, EARLY // 2, EARLY, EARLY)
    close(1, sums)
    for k in range(CHUNKS):
        start(read(0, k, CHUNKS))
    held[1][z] = part[1][...]
    pl.semaphore_wait(barrier, n_zero - 1)
    key_copies = exchange(1, part[1], held[1])
    sums = tally(2, sums_start(2), 0, EARLY, EARLY)
    close(2, sums)
    held[2][z] = part[2][...]
    value_copies = exchange(2, part[2], held[2])
    norm_copies = exchange(3, norm, gain_ref)
    norm_copies.append(pltpu.make_async_copy(norm, gain_ref.at[z], norm_sem))
    norm_copies[-1].start()
    sums = tally(0, sums_start(0), 0, CHUNKS // SPLIT * 3, CHUNKS)
    scale = settle(1, key_copies)
    narrow_rows(fresh[1], own[1], scale, 0, rows)
    launch(0)
    sums = tally(0, sums, CHUNKS // SPLIT * 3, CHUNKS, CHUNKS)
    close(0, sums)
    held[0][z] = part[0][...]
    query_copies = exchange(0, part[0], held[0])
    scale = settle(2, value_copies)
    narrow_rows(fresh[2], own[2], scale, 0, rows)
    launch(1)
    scale = settle(0, query_copies)
    for p in range(2, len(pieces)):
        narrow_rows(fresh[0], own[0], scale, pieces[p][1], pieces[p][2])
        launch(p)

    def relay(hop, carry):
        for p in range(len(pieces)):
            for way in (0, 1):
                owner = lax.rem(z + (n_zero - hop if way == 0 else hop), n_zero)
                before = lax.rem(z + (n_zero - hop + 1 if way == 0 else hop - 1), n_zero)

                @pl.when(arrives(p, hop - 1, way))
                def _():
                    move(p, hop - 1, way, owner).wait_recv()

                @pl.when(sends(p, hop, way))
                def _():
                    @pl.when(sends(p, hop - 1, way))
                    def _():
                        move(p, hop - 1, way, before).wait_send()

                    move(p, hop, way, owner).start()

        return carry

    lax.fori_loop(1, n_zero, relay, 0)
    for p in range(len(pieces)):
        for way in (0, 1):
            rank = ranks[way]

            @pl.when(sends(p, rank, way))
            def _():
                move(p, 0, way, z).wait_send()

    for p in range(len(pieces)):
        finish(own_copies(p))
    finish(norm_copies)


def carry(n_zero, pieces, arrays, share, train, step):
    vmem = pl.BlockSpec(memory_space=pltpu.VMEM)
    hbm = pl.BlockSpec(memory_space=pl.ANY)
    shapes = [array.shape for array in arrays[::2]]
    rows = shapes[0][0]
    parts = [(1, width) for _, width in shapes]
    lates = [(count, shapes[which][1]) for which, _, count, late in pieces if late]
    count = len(pieces)
    return pl.pallas_call(
        functools.partial(carry_kernel, n_zero, pieces),
        out_shape=(
            *(jax.ShapeDtypeStruct((n_zero * rows, width), jnp.bfloat16) for _, width in shapes),
            *(jax.ShapeDtypeStruct(part, jnp.float32) for part in parts),
            jax.ShapeDtypeStruct((n_zero,) + train.shape, jnp.bfloat16),
            *(jax.ShapeDtypeStruct(shape, jnp.bfloat16) for shape in lates),
        ),
        in_specs=[hbm] * 6 + [vmem] * 3,
        out_specs=(*[hbm] * 3, *[vmem] * 4, *[hbm] * len(lates)),
        scratch_shapes=[
            *(pltpu.VMEM(shape, jnp.float32) for shape in shapes),
            *(pltpu.VMEM(shape, jnp.float32) for shape in shapes),
            *(pltpu.VMEM(shape, jnp.bfloat16) for shape in shapes),
            pltpu.VMEM((rows, LANES), jnp.float32),
            pltpu.VMEM(train.shape, jnp.bfloat16),
            *(pltpu.VMEM((n_zero,) + part, jnp.float32) for part in parts),
            *(pltpu.VMEM(part, jnp.float32) for part in parts),
            pltpu.SemaphoreType.DMA((3, 2, CHUNKS)),
            pltpu.SemaphoreType.DMA((count,)),
            pltpu.SemaphoreType.DMA((LATE,)),
            pltpu.SemaphoreType.DMA((4, n_zero)),
            pltpu.SemaphoreType.DMA((4, n_zero)),
            pltpu.SemaphoreType.DMA,
            pltpu.SemaphoreType.DMA((2, count)),
            pltpu.SemaphoreType.DMA((2, n_zero, count)),
        ],
        compiler_params=pltpu.CompilerParams(
            collective_id=0, has_side_effects=True, vmem_limit_bytes=60 * 2**20
        ),
        name="carry",
    )(*arrays, share, train, step)


def spread_kernel(n_model, part_ref, all_ref, sent, got, own):
    m = lax.axis_index("model")
    barrier = pltpu.get_barrier_semaphore()
    peers = [lax.rem(m + k, n_model) for k in range(1, n_model)]
    for peer in peers:
        pl.semaphore_signal(barrier, inc=1, device_id={"model": peer}, device_id_type=MESH)
    mine = pltpu.make_async_copy(part_ref, all_ref.at[m], own)
    mine.start()
    pl.semaphore_wait(barrier, n_model - 1)
    copies = []
    for k, peer in enumerate(peers, 1):
        copies.append(
            pltpu.make_async_remote_copy(
                src_ref=part_ref,
                dst_ref=all_ref.at[m],
                send_sem=sent.at[k],
                recv_sem=got.at[k],
                device_id={"model": peer},
                device_id_type=MESH,
            )
        )
    for copy in copies:
        copy.start()
    for copy in copies + [mine]:
        copy.wait()


def spread(n_model, part):
    vmem = pl.BlockSpec(memory_space=pltpu.VMEM)
    return pl.pallas_call(
        functools.partial(spread_kernel, n_model),
        out_shape=jax.ShapeDtypeStruct((n_model,) + part.shape, part.dtype),
        in_specs=[vmem],
        out_specs=vmem,
        scratch_shapes=[
            pltpu.SemaphoreType.DMA((n_model,)),
            pltpu.SemaphoreType.DMA((n_model,)),
            pltpu.SemaphoreType.DMA,
        ],
        compiler_params=pltpu.CompilerParams(collective_id=1, has_side_effects=True),
        cost_estimate=pl.CostEstimate(flops=20_000_000, bytes_accessed=65536, transcendentals=0),
        name="spread",
    )(part)


def settle_kernel(source, target):
    target[...] = source[...]


def settle(array):
    rows, width = array.shape
    block = rows // 16
    spec = pl.BlockSpec((block, width), lambda i: (i, 0))
    return pl.pallas_call(
        settle_kernel,
        out_shape=jax.ShapeDtypeStruct(array.shape, array.dtype),
        grid=(16,),
        in_specs=[spec],
        out_specs=spec,
        cost_estimate=pl.CostEstimate(
            flops=8 * rows * width, bytes_accessed=4 * rows * width, transcendentals=0
        ),
        name="settle",
    )(array)


def on_device(n_zero, n_model, *args):
    arrays = args[:6]
    mix_share, norm_train, norm_step = args[6:]
    rows = mix_share.shape[0]
    z = lax.axis_index("zero")
    pieces = [(1, 0, rows, 0), (2, 0, rows, 0)]
    for k, (low, high) in enumerate(zip(CUTS[:-1], CUTS[1:])):
        late = max(0, k + 1 + LATE - (len(CUTS) - 1))
        pieces.append((0, low * rows // CUTS[-1], (high - low) * rows // CUTS[-1], late))
    results = carry(
        n_zero,
        tuple(pieces),
        arrays,
        mix_share.reshape(-1, LANES),
        norm_train[None, :],
        norm_step[None, :],
    )
    serve, totals, gain, lates = list(results[:3]), results[3:6], results[6], results[7:]
    swap = [(k, k ^ 1) for k in range(n_zero)]
    moved = []
    for k, block in enumerate(lates):
        with jax.named_scope(f"late_{k}"):
            moved.append(lax.ppermute(block, "zero", swap))
    serve = [settle(array) for array in serve]
    partner = z + 1 - 2 * lax.rem(z, 2)
    for block, (which, low, _, late) in zip(moved, pieces[-LATE:]):
        serve[which] = lax.dynamic_update_slice(
            serve[which], block, (partner * rows + low, jnp.zeros_like(z))
        )
    totals, gain, _ = lax.optimization_barrier((totals, gain, serve[1]))
    factors = [jnp.sqrt(total[0]) for total in totals]
    gain = spread(n_model, gain)
    gain = gain.reshape(n_model, n_zero, -1).transpose(1, 0, 2)
    return (*serve, *factors, gain.reshape(-1))


def solution(mesh):
    in_specs = (
        P(("unit", "zero"), "model"),
        P(("unit", "zero"), "model"),
        P(("unit", "zero"), "model"),
        P(("unit", "zero"), "model"),
        P(("unit", "zero"), "model"),
        P(("unit", "zero"), "model"),
        P(("unit", "zero")),
        P(("unit", "zero", "model")),
        P(("unit", "zero", "model")),
    )
    out_specs = (
        P("unit", "model"),
        P("unit", "model"),
        P("unit", "model"),
        P(("unit", "model")),
        P(("unit", "model")),
        P(("unit", "model")),
        P("unit"),
    )
    return jax.shard_map(
        functools.partial(on_device, mesh.shape["zero"], mesh.shape["model"]),
        mesh=mesh,
        in_specs=in_specs,
        out_specs=out_specs,
        check_vma=False,
    )
```

```python
import functools

import jax
import jax.numpy as jnp
from jax import lax
from jax.experimental import pallas as pl
from jax.experimental.pallas import tpu as pltpu
from jax.sharding import PartitionSpec as P

MESH = pl.DeviceIdType.MESH
LANES = 128
GROUP = 32
EARLY = 8
CHUNKS = 16
HEAD = 3
CUTS = (0, 8, 16, 22, 24, 31, 32)
LATES = (0, 0, 0, 2, 1, 3)
LATE = 3
STAGGER = 2
COPIES = (16, 4, 4)
SLOTS = (8, 4, 4)
LAG = 4


def total_of(held, n_zero):
    total = held[0]
    for k in range(1, n_zero):
        total = total + held[k]
    return total


def slabs_of(width):
    return [(low, min(LANES, width - low)) for low in range(0, width, LANES)]


def mix_rows(first, second, wide, low, count, sums):
    group = min(GROUP, count)
    slabs = slabs_of(first.shape[1])

    def step(i, sums):
        here = pl.ds(pl.multiple_of(low + i * group, group), group)
        share = wide[here, :]
        rest = 1.0 - share
        out = []
        for (start, size), total in zip(slabs, sums):
            columns = pl.ds(start, size)
            fresh = share[:, :size] * first[here, columns] + rest[:, :size] * second[here, columns]
            first[here, columns] = fresh
            out.append(total + jnp.sum((fresh * fresh).reshape(group // 8, 8, size), axis=0))
        return tuple(out)

    return lax.fori_loop(0, count // group, step, tuple(sums))


def narrow_rows(fresh, own, scale, low, count):
    group = min(GROUP, count)
    slabs = slabs_of(fresh.shape[1])
    scales = [jnp.broadcast_to(scale[:, start : start + size], (group, size)) for start, size in slabs]

    def step(i, carry):
        here = pl.ds(pl.multiple_of(low + i * group, group), group)
        for (start, size), factor in zip(slabs, scales):
            columns = pl.ds(start, size)
            own[here, columns] = (fresh[here, columns] * factor).astype(own.dtype)
        return carry

    lax.fori_loop(0, count // group, step, 0)


def carry_kernel(n_zero, pieces, *refs):
    inputs, outputs, scratch = refs[:9], refs[9 : 16 + LATE], refs[16 + LATE :]
    sources = (inputs[0:2], inputs[2:4], inputs[4:6])
    share_ref, train_ref, step_ref = inputs[6:]
    serve, totals, gain_ref = outputs[0:3], outputs[3:6], outputs[6]
    late_refs = outputs[7:]
    fresh, second, own = scratch[0:3], scratch[3:6], scratch[6:9]
    wide, norm = scratch[9:11]
    held, part = scratch[11:14], scratch[14:17]
    read_sem, own_sem, late_sem, stat_sent, stat_got, norm_sem, sent, got = scratch[17:]

    z = lax.axis_index("zero")
    lead_unit = lax.axis_index("unit") == 0
    rows = fresh[0].shape[0]
    barrier = pltpu.get_barrier_semaphore()
    peers = [lax.rem(z + k, n_zero) for k in range(1, n_zero)]
    for peer in peers:
        pl.semaphore_signal(barrier, inc=1, device_id={"zero": peer}, device_id_type=MESH)

    def read(which, k, chunks):
        step = rows // chunks
        here = pl.ds(k * step, step)
        return [
            pltpu.make_async_copy(source.at[here], target.at[here], read_sem.at[which, side, k])
            for side, (source, target) in enumerate(zip(sources[which], (fresh[which], second[which])))
        ]

    def start(copies):
        for copy in copies:
            copy.start()

    def finish(copies):
        for copy in copies:
            copy.wait()

    for k in range(EARLY):
        start(read(1, k, EARLY))
    norm[...] = (train_ref[...] + step_ref[...]).astype(norm.dtype)
    for k in range(rows // LANES):
        line = jnp.broadcast_to(share_ref[k : k + 1, :], (LANES, LANES))
        wide[k * LANES : (k + 1) * LANES, :] = jnp.transpose(line)

    def sums_start(which):
        return tuple(jnp.zeros((8, size), jnp.float32) for _, size in slabs_of(fresh[which].shape[1]))

    def tally(which, sums, low, high, chunks):
        step = rows // chunks
        for k in range(low, high):
            finish(read(which, k, chunks))
            sums = mix_rows(fresh[which], second[which], wide, k * step, step, sums)
        return sums

    def close(which, sums):
        for (start_at, size), value in zip(slabs_of(fresh[which].shape[1]), sums):
            part[which][:, start_at : start_at + size] = jnp.sum(value, axis=0, keepdims=True)

    def exchange(index, source, target):
        copies = []
        for k, peer in enumerate(peers, 1):
            copies.append(
                pltpu.make_async_remote_copy(
                    src_ref=source,
                    dst_ref=target.at[z],
                    send_sem=stat_sent.at[index, k],
                    recv_sem=stat_got.at[index, k],
                    device_id={"zero": peer},
                    device_id_type=MESH,
                )
            )
        start(copies)
        return copies

    def move(p, hop, way, owner, source=None):
        which, low, count, _ = pieces[p]
        here = pl.ds(pl.multiple_of(owner * rows + low, 8), count)
        target = serve[which].at[here]
        return pltpu.make_async_remote_copy(
            src_ref=target if source is None else source,
            dst_ref=target,
            send_sem=sent.at[way, p],
            recv_sem=got.at[way, hop, p],
            device_id={"zero": lax.rem(z + (1 if way == 0 else n_zero - 1), n_zero)},
            device_id_type=MESH,
        )

    ranks = (z, n_zero - 1 - z)

    def kept(p, hop, rank, last):
        skip = jnp.logical_and(hop == 0, rank == last)
        if pieces[p][3] == STAGGER:
            skip = jnp.logical_and(skip, lead_unit)
        return jnp.logical_not(skip)

    def sends(p, hop, way):
        rank = ranks[way]
        yes = jnp.logical_and(rank < n_zero - 1, rank >= hop)
        if pieces[p][3]:
            yes = jnp.logical_and(yes, kept(p, hop, rank, n_zero - 2))
        return yes

    def arrives(p, hop, way):
        rank = ranks[way]
        yes = rank >= hop + 1
        if pieces[p][3]:
            yes = jnp.logical_and(yes, kept(p, hop, rank, n_zero - 1))
        return yes

    def own_copies(p):
        which, low, count, late = pieces[p]
        source = own[which].at[pl.ds(low, count)]
        here = pl.ds(pl.multiple_of(z * rows + low, 8), count)
        copies = [pltpu.make_async_copy(source, serve[which].at[here], own_sem.at[p])]
        if late:
            copies.append(pltpu.make_async_copy(source, late_refs[late - 1], late_sem.at[late - 1]))
        return copies

    def first_move(p, way):
        which, low, count, _ = pieces[p]
        return move(p, 0, way, z, own[which].at[pl.ds(low, count)])

    def launch(p):
        for way in (0, 1):

            @pl.when(sends(p, 0, way))
            def _():
                first_move(p, way).start()

        start(own_copies(p))

    def settle(which, copies):
        finish(copies)
        total = total_of(held[which], n_zero)
        totals[which][...] = total
        return 1.0 / jnp.sqrt(total)

    def send_own(which, scale):
        for p, (owner, low, count, _) in enumerate(pieces):
            if owner == which:
                narrow_rows(fresh[which], own[which], scale, low, count)
                launch(p)

    sums = tally(1, sums_start(1), 0, EARLY // 2, EARLY)
    for k in range(EARLY):
        start(read(2, k, EARLY))
    sums = tally(1, sums, EARLY // 2, EARLY, EARLY)
    close(1, sums)
    for k in range(CHUNKS):
        start(read(0, k, CHUNKS))
    held[1][z] = part[1][...]
    pl.semaphore_wait(barrier, n_zero - 1)
    key_copies = exchange(1, part[1], held[1])
    sums = tally(2, sums_start(2), 0, EARLY, EARLY)
    close(2, sums)
    held[2][z] = part[2][...]
    value_copies = exchange(2, part[2], held[2])
    norm_copies = exchange(3, norm, gain_ref)
    norm_copies.append(pltpu.make_async_copy(norm, gain_ref.at[z], norm_sem))
    norm_copies[-1].start()
    sums = tally(0, sums_start(0), 0, HEAD, CHUNKS)
    scale = settle(1, key_copies)
    send_own(1, scale)
    sums = tally(0, sums, HEAD, CHUNKS, CHUNKS)
    close(0, sums)
    held[0][z] = part[0][...]
    query_copies = exchange(0, part[0], held[0])
    scale = settle(2, value_copies)
    send_own(2, scale)
    scale = settle(0, query_copies)
    send_own(0, scale)

    def relay(hop, carry):
        for p in range(len(pieces)):
            for way in (0, 1):
                owner = lax.rem(z + (n_zero - hop if way == 0 else hop), n_zero)
                before = lax.rem(z + (n_zero - hop + 1 if way == 0 else hop - 1), n_zero)

                @pl.when(arrives(p, hop - 1, way))
                def _():
                    move(p, hop - 1, way, owner).wait_recv()

                @pl.when(sends(p, hop, way))
                def _():
                    @pl.when(sends(p, hop - 1, way))
                    def _():
                        move(p, hop - 1, way, before).wait_send()

                    move(p, hop, way, owner).start()

        return carry

    lax.fori_loop(1, n_zero, relay, 0)
    for p in range(len(pieces)):
        for way in (0, 1):
            rank = ranks[way]

            @pl.when(sends(p, rank, way))
            def _():
                move(p, 0, way, z).wait_send()

    for p in range(len(pieces)):
        finish(own_copies(p))
    finish(norm_copies)


def carry(n_zero, pieces, arrays, share, train, step):
    vmem = pl.BlockSpec(memory_space=pltpu.VMEM)
    hbm = pl.BlockSpec(memory_space=pl.ANY)
    shapes = [array.shape for array in arrays[::2]]
    rows = shapes[0][0]
    parts = [(1, width) for _, width in shapes]
    lates = [(count, shapes[which][1]) for which, _, count, late in sorted(pieces, key=lambda p: p[3]) if late]
    count = len(pieces)
    return pl.pallas_call(
        functools.partial(carry_kernel, n_zero, pieces),
        out_shape=(
            *(jax.ShapeDtypeStruct((n_zero * rows, width), jnp.bfloat16) for _, width in shapes),
            *(jax.ShapeDtypeStruct(part, jnp.float32) for part in parts),
            jax.ShapeDtypeStruct((n_zero,) + train.shape, jnp.bfloat16),
            *(jax.ShapeDtypeStruct(shape, jnp.bfloat16) for shape in lates),
        ),
        in_specs=[hbm] * 6 + [vmem] * 3,
        out_specs=(*[hbm] * 3, *[vmem] * 4, *[hbm] * len(lates)),
        scratch_shapes=[
            *(pltpu.VMEM(shape, jnp.float32) for shape in shapes),
            *(pltpu.VMEM(shape, jnp.float32) for shape in shapes),
            *(pltpu.VMEM(shape, jnp.bfloat16) for shape in shapes),
            pltpu.VMEM((rows, LANES), jnp.float32),
            pltpu.VMEM(train.shape, jnp.bfloat16),
            *(pltpu.VMEM((n_zero,) + part, jnp.float32) for part in parts),
            *(pltpu.VMEM(part, jnp.float32) for part in parts),
            pltpu.SemaphoreType.DMA((3, 2, CHUNKS)),
            pltpu.SemaphoreType.DMA((count,)),
            pltpu.SemaphoreType.DMA((LATE,)),
            pltpu.SemaphoreType.DMA((4, n_zero)),
            pltpu.SemaphoreType.DMA((4, n_zero)),
            pltpu.SemaphoreType.DMA,
            pltpu.SemaphoreType.DMA((2, count)),
            pltpu.SemaphoreType.DMA((2, n_zero, count)),
        ],
        compiler_params=pltpu.CompilerParams(
            collective_id=0, has_side_effects=True, vmem_limit_bytes=60 * 2**20
        ),
        name="carry",
    )(*arrays, share, train, step)


def spread_kernel(n_model, part_ref, all_ref, sent, got, own):
    m = lax.axis_index("model")
    barrier = pltpu.get_barrier_semaphore()
    peers = [lax.rem(m + k, n_model) for k in range(1, n_model)]
    for peer in peers:
        pl.semaphore_signal(barrier, inc=1, device_id={"model": peer}, device_id_type=MESH)
    mine = pltpu.make_async_copy(part_ref, all_ref.at[m], own)
    mine.start()
    pl.semaphore_wait(barrier, n_model - 1)
    copies = []
    for k, peer in enumerate(peers, 1):
        copies.append(
            pltpu.make_async_remote_copy(
                src_ref=part_ref,
                dst_ref=all_ref.at[m],
                send_sem=sent.at[k],
                recv_sem=got.at[k],
                device_id={"model": peer},
                device_id_type=MESH,
            )
        )
    for copy in copies:
        copy.start()
    for copy in copies + [mine]:
        copy.wait()


def spread(n_model, part):
    vmem = pl.BlockSpec(memory_space=pltpu.VMEM)
    return pl.pallas_call(
        functools.partial(spread_kernel, n_model),
        out_shape=jax.ShapeDtypeStruct((n_model,) + part.shape, part.dtype),
        in_specs=[vmem],
        out_specs=vmem,
        scratch_shapes=[
            pltpu.SemaphoreType.DMA((n_model,)),
            pltpu.SemaphoreType.DMA((n_model,)),
            pltpu.SemaphoreType.DMA,
        ],
        compiler_params=pltpu.CompilerParams(collective_id=1, has_side_effects=True),
        cost_estimate=pl.CostEstimate(flops=20_000_000, bytes_accessed=65536, transcendentals=0),
        name="spread",
    )(part)


def settle_kernel(plan, *refs):
    sources, targets, spaces = refs[0:3], refs[3:6], refs[6:9]
    read_sem, write_sem = refs[9:]

    def reading(i):
        which, low, count, slot, _ = plan[i]
        return pltpu.make_async_copy(sources[which].at[pl.ds(low, count)], spaces[which].at[slot], read_sem.at[i])

    def writing(i):
        which, low, count, slot, _ = plan[i]
        return pltpu.make_async_copy(spaces[which].at[slot], targets[which].at[pl.ds(low, count)], write_sem.at[i])

    def read_after(i):
        for k, step in enumerate(plan):
            if step[4] == i:
                reading(k).start()

    read_after(None)
    for i in range(len(plan)):
        reading(i).wait()
        writing(i).start()
        if i >= LAG:
            writing(i - LAG).wait()
            read_after(i - LAG)
    for i in range(max(0, len(plan) - LAG), len(plan)):
        writing(i).wait()


def settle(arrays):
    plan, spaces = [], []
    for which in (1, 2, 0):
        step = arrays[which].shape[0] // COPIES[which]
        first = len(plan)
        for k in range(COPIES[which]):
            after = first + k - SLOTS[which] if k >= SLOTS[which] else None
            plan.append((which, k * step, step, k % SLOTS[which], after))
    for which, array in enumerate(arrays):
        step = array.shape[0] // COPIES[which]
        spaces.append(pltpu.VMEM((SLOTS[which], step, array.shape[1]), array.dtype))
    hbm = pl.BlockSpec(memory_space=pl.ANY)
    size = sum(array.shape[0] * array.shape[1] for array in arrays)
    return pl.pallas_call(
        functools.partial(settle_kernel, tuple(plan)),
        out_shape=tuple(jax.ShapeDtypeStruct(array.shape, array.dtype) for array in arrays),
        in_specs=[hbm] * 3,
        out_specs=(hbm,) * 3,
        scratch_shapes=spaces
        + [pltpu.SemaphoreType.DMA((len(plan),)), pltpu.SemaphoreType.DMA((len(plan),))],
        compiler_params=pltpu.CompilerParams(vmem_limit_bytes=40 * 2**20),
        cost_estimate=pl.CostEstimate(flops=8 * size, bytes_accessed=4 * size, transcendentals=0),
        name="settle",
    )(*arrays)


def on_device(n_zero, n_model, *args):
    arrays = args[:6]
    mix_share, norm_train, norm_step = args[6:]
    rows = mix_share.shape[0]
    z, unit = lax.axis_index("zero"), lax.axis_index("unit")
    pieces = [(1, 0, rows // 4, 0), (1, rows // 4, rows - rows // 4, 0), (2, 0, rows, 0)]
    bounds = [cut * rows // CUTS[-1] for cut in CUTS]
    for k, late in enumerate(LATES):
        pieces.append((0, bounds[k], bounds[k + 1] - bounds[k], late))
    results = carry(
        n_zero,
        tuple(pieces),
        arrays,
        mix_share.reshape(-1, LANES),
        norm_train[None, :],
        norm_step[None, :],
    )
    serve, totals, gain, lates = list(results[:3]), results[3:6], results[6], results[7:]
    swap = [(k, k ^ 1) for k in range(n_zero)]
    partner = z + 1 - 2 * lax.rem(z, 2)
    landed = serve[0]
    serve = list(settle(serve))
    for late in range(1, LATE + 1):
        _, low, count, _ = pieces[LATES.index(late) - len(LATES)]
        where = (partner * rows + low, jnp.zeros_like(z))
        if late != STAGGER:
            block = lax.ppermute(lates[late - 1], "zero", swap)
        else:
            block = lax.ppermute(lates[late - 1], ("unit", "zero"), swap)
            there = lax.dynamic_slice(landed, where, (count, landed.shape[1]))
            block = jnp.where(unit == 0, block, there)
        serve[0] = lax.dynamic_update_slice(serve[0], block, where)
    totals, gain, _ = lax.optimization_barrier((totals, gain, serve[1]))
    factors = [jnp.sqrt(total[0]) for total in totals]
    gain = spread(n_model, gain)
    gain = gain.reshape(n_model, n_zero, -1).transpose(1, 0, 2)
    return (*serve, *factors, gain.reshape(-1))


def solution(mesh):
    in_specs = (
        P(("unit", "zero"), "model"),
        P(("unit", "zero"), "model"),
        P(("unit", "zero"), "model"),
        P(("unit", "zero"), "model"),
        P(("unit", "zero"), "model"),
        P(("unit", "zero"), "model"),
        P(("unit", "zero")),
        P(("unit", "zero", "model")),
        P(("unit", "zero", "model")),
    )
    out_specs = (
        P("unit", "model"),
        P("unit", "model"),
        P("unit", "model"),
        P(("unit", "model")),
        P(("unit", "model")),
        P(("unit", "model")),
        P("unit"),
    )
    return jax.shard_map(
        functools.partial(on_device, mesh.shape["zero"], mesh.shape["model"]),
        mesh=mesh,
        in_specs=in_specs,
        out_specs=out_specs,
        check_vma=False,
    )
```

```python
import functools
import math

import jax
import jax.numpy as jnp
from jax import lax
from jax.experimental import pallas as pl
from jax.experimental.pallas import tpu as pltpu
from jax.sharding import PartitionSpec as P

MESH = pl.DeviceIdType.MESH
LANES = 128
GROUP = 32
EARLY = 8
CHUNKS = 16
HEAD = 3
CUTS = (0, 8, 16, 22, 24, 31, 32)
LATES = (0, 0, 0, 2, 1, 3)
LATE = 3
STAGGER = 2
RAW = -1
COPIES = (16, 4, 4)
SLOTS = (8, 4, 4)
LAG = 4


def total_of(held, n_zero):
    total = held[0]
    for k in range(1, n_zero):
        total = total + held[k]
    return total


def slabs_of(width):
    return [(low, min(LANES, width - low)) for low in range(0, width, LANES)]


def mix_rows(first, second, wide, low, count, sums):
    group = math.gcd(GROUP, count)
    slabs = slabs_of(first.shape[1])

    def step(i, sums):
        here = pl.ds(pl.multiple_of(low + i * group, group), group)
        share = wide[here, :]
        rest = 1.0 - share
        out = []
        for (start, size), total in zip(slabs, sums):
            columns = pl.ds(start, size)
            fresh = share[:, :size] * first[here, columns] + rest[:, :size] * second[here, columns]
            first[here, columns] = fresh
            out.append(total + jnp.sum((fresh * fresh).reshape(group // 8, 8, size), axis=0))
        return tuple(out)

    return lax.fori_loop(0, count // group, step, tuple(sums))


def narrow_rows(fresh, own, scale, low, count):
    group = math.gcd(GROUP, count)
    slabs = slabs_of(fresh.shape[1])
    scales = [jnp.broadcast_to(scale[:, start : start + size], (group, size)) for start, size in slabs]

    def step(i, carry):
        here = pl.ds(pl.multiple_of(low + i * group, group), group)
        for (start, size), factor in zip(slabs, scales):
            columns = pl.ds(start, size)
            own[here, columns] = (fresh[here, columns] * factor).astype(own.dtype)
        return carry

    lax.fori_loop(0, count // group, step, 0)


def carry_kernel(n_zero, pieces, *refs):
    inputs, outputs, scratch = refs[:9], refs[9 : 16 + LATE], refs[16 + LATE :]
    sources = (inputs[0:2], inputs[2:4], inputs[4:6])
    share_ref, train_ref, step_ref = inputs[6:]
    serve, totals, gain_ref = outputs[0:3], outputs[3:6], outputs[6]
    late_refs = outputs[7:]
    fresh, second, own = scratch[0:3], scratch[3:6], scratch[6:9]
    wide, norm = scratch[9:11]
    held, part = scratch[11:14], scratch[14:17]
    raw_held, raw_own = scratch[17:19]
    read_sem, own_sem, late_sem, stat_sent, stat_got, norm_sem, sent, got, raw_sem = scratch[19:]

    z = lax.axis_index("zero")
    lead_unit = lax.axis_index("unit") == 0
    rows = fresh[0].shape[0]
    barrier = pltpu.get_barrier_semaphore()
    peers = [lax.rem(z + k, n_zero) for k in range(1, n_zero)]
    for peer in peers:
        pl.semaphore_signal(barrier, inc=1, device_id={"zero": peer}, device_id_type=MESH)

    def read(which, k, chunks):
        step = rows // chunks
        here = pl.ds(k * step, step)
        return [
            pltpu.make_async_copy(source.at[here], target.at[here], read_sem.at[which, side, k])
            for side, (source, target) in enumerate(zip(sources[which], (fresh[which], second[which])))
        ]

    def start(copies):
        for copy in copies:
            copy.start()

    def finish(copies):
        for copy in copies:
            copy.wait()

    for k in range(EARLY):
        start(read(1, k, EARLY))
    norm[...] = (train_ref[...] + step_ref[...]).astype(norm.dtype)
    for k in range(rows // LANES):
        line = jnp.broadcast_to(share_ref[k : k + 1, :], (LANES, LANES))
        wide[k * LANES : (k + 1) * LANES, :] = jnp.transpose(line)

    def sums_start(which):
        return tuple(jnp.zeros((8, size), jnp.float32) for _, size in slabs_of(fresh[which].shape[1]))

    def tally(which, sums, low, high, chunks):
        step = rows // chunks
        for k in range(low, high):
            finish(read(which, k, chunks))
            sums = mix_rows(fresh[which], second[which], wide, k * step, step, sums)
        return sums

    def close(which, sums):
        for (start_at, size), value in zip(slabs_of(fresh[which].shape[1]), sums):
            part[which][:, start_at : start_at + size] = jnp.sum(value, axis=0, keepdims=True)

    def exchange(index, source, target):
        copies = []
        for k, peer in enumerate(peers, 1):
            copies.append(
                pltpu.make_async_remote_copy(
                    src_ref=source,
                    dst_ref=target.at[z],
                    send_sem=stat_sent.at[index, k],
                    recv_sem=stat_got.at[index, k],
                    device_id={"zero": peer},
                    device_id_type=MESH,
                )
            )
        start(copies)
        return copies

    def move(p, hop, way, owner, source=None):
        which, low, count, _ = pieces[p]
        here = pl.ds(pl.multiple_of(owner * rows + low, 8), count)
        target = serve[which].at[here]
        return pltpu.make_async_remote_copy(
            src_ref=target if source is None else source,
            dst_ref=target,
            send_sem=sent.at[way, p],
            recv_sem=got.at[way, hop, p],
            device_id={"zero": lax.rem(z + (1 if way == 0 else n_zero - 1), n_zero)},
            device_id_type=MESH,
        )

    ranks = (z, n_zero - 1 - z)

    def kept(p, hop, rank, last):
        skip = jnp.logical_and(hop == 0, rank == last)
        if pieces[p][3] == STAGGER:
            skip = jnp.logical_and(skip, lead_unit)
        return jnp.logical_not(skip)

    def sends(p, hop, way):
        rank = ranks[way]
        yes = jnp.logical_and(rank < n_zero - 1, rank >= hop)
        if pieces[p][3] == RAW:
            yes = jnp.logical_and(yes, hop >= 1)
        elif pieces[p][3]:
            yes = jnp.logical_and(yes, kept(p, hop, rank, n_zero - 2))
        return yes

    def arrives(p, hop, way):
        rank = ranks[way]
        yes = rank >= hop + 1
        if pieces[p][3] == RAW:
            yes = jnp.logical_and(yes, hop >= 1)
        elif pieces[p][3]:
            yes = jnp.logical_and(yes, kept(p, hop, rank, n_zero - 1))
        return yes

    def own_copies(p):
        which, low, count, late = pieces[p]
        source = own[which].at[pl.ds(low, count)]
        here = pl.ds(pl.multiple_of(z * rows + low, 8), count)
        copies = [pltpu.make_async_copy(source, serve[which].at[here], own_sem.at[p])]
        if late > 0:
            copies.append(pltpu.make_async_copy(source, late_refs[late - 1], late_sem.at[late - 1]))
        return copies

    def first_move(p, way):
        which, low, count, _ = pieces[p]
        return move(p, 0, way, z, own[which].at[pl.ds(low, count)])

    def launch(p):
        if pieces[p][3] != RAW:
            for way in (0, 1):

                @pl.when(sends(p, 0, way))
                def _():
                    first_move(p, way).start()

        start(own_copies(p))

    raw = [p for p, piece in enumerate(pieces) if piece[3] == RAW][0]
    raw_which, raw_low, raw_count, _ = pieces[raw]

    def raw_move(way):
        return pltpu.make_async_remote_copy(
            src_ref=fresh[raw_which].at[pl.ds(raw_low, raw_count)],
            dst_ref=raw_held.at[way],
            send_sem=raw_sem.at[0, way],
            recv_sem=raw_sem.at[1, way],
            device_id={"zero": lax.rem(z + (1 if way == 0 else n_zero - 1), n_zero)},
            device_id_type=MESH,
        )

    def raw_copy(way):
        owner = lax.rem(z + (n_zero - 1 if way == 0 else 1), n_zero)
        here = pl.ds(pl.multiple_of(owner * rows + raw_low, 8), raw_count)
        return pltpu.make_async_copy(raw_own.at[way], serve[raw_which].at[here], raw_sem.at[2, way])

    def settle(which, copies):
        finish(copies)
        total = total_of(held[which], n_zero)
        totals[which][...] = total
        return 1.0 / jnp.sqrt(total)

    def send_own(which, scale):
        for p, (owner, low, count, late) in sorted(enumerate(pieces), key=lambda item: item[1][3] == RAW):
            if owner == which:
                narrow_rows(fresh[which], own[which], scale, low, count)
                launch(p)

    sums = tally(1, sums_start(1), 0, EARLY // 2, EARLY)
    for k in range(EARLY):
        start(read(2, k, EARLY))
    sums = tally(1, sums, EARLY // 2, EARLY, EARLY)
    close(1, sums)
    for k in range(CHUNKS):
        start(read(0, k, CHUNKS))
    held[1][z] = part[1][...]
    pl.semaphore_wait(barrier, n_zero - 1)
    key_copies = exchange(1, part[1], held[1])
    for way in (0, 1):

        @pl.when(ranks[way] < n_zero - 1)
        def _():
            raw_move(way).start()

    sums = tally(2, sums_start(2), 0, EARLY, EARLY)
    close(2, sums)
    held[2][z] = part[2][...]
    value_copies = exchange(2, part[2], held[2])
    norm_copies = exchange(3, norm, gain_ref)
    norm_copies.append(pltpu.make_async_copy(norm, gain_ref.at[z], norm_sem))
    norm_copies[-1].start()
    sums = tally(0, sums_start(0), 0, HEAD, CHUNKS)
    scale = settle(1, key_copies)
    send_own(1, scale)
    for way in (0, 1):

        @pl.when(ranks[way] >= 1)
        def _():
            raw_move(way).wait_recv()
            narrow_rows(raw_held.at[way], raw_own.at[way], scale, 0, raw_count)
            raw_copy(way).start()

    sums = tally(0, sums, HEAD, CHUNKS, CHUNKS)
    close(0, sums)
    held[0][z] = part[0][...]
    query_copies = exchange(0, part[0], held[0])
    scale = settle(2, value_copies)
    send_own(2, scale)
    scale = settle(0, query_copies)
    send_own(0, scale)

    def relay(hop, carry):
        for p in range(len(pieces)):
            for way in (0, 1):
                owner = lax.rem(z + (n_zero - hop if way == 0 else hop), n_zero)
                before = lax.rem(z + (n_zero - hop + 1 if way == 0 else hop - 1), n_zero)

                @pl.when(arrives(p, hop - 1, way))
                def _():
                    move(p, hop - 1, way, owner).wait_recv()

                @pl.when(sends(p, hop, way))
                def _():
                    @pl.when(sends(p, hop - 1, way))
                    def _():
                        move(p, hop - 1, way, before).wait_send()

                    move(p, hop, way, owner).start()

        return carry

    for way in (0, 1):

        @pl.when(ranks[way] >= 1)
        def _():
            raw_copy(way).wait()

        @pl.when(ranks[way] < n_zero - 1)
        def _():
            raw_move(way).wait_send()

    lax.fori_loop(1, n_zero, relay, 0)
    for p in range(len(pieces)):
        for way in (0, 1):
            rank = ranks[way]

            @pl.when(sends(p, rank, way))
            def _():
                move(p, 0, way, z).wait_send()

    for p in range(len(pieces)):
        finish(own_copies(p))
    finish(norm_copies)


def carry(n_zero, pieces, arrays, share, train, step):
    vmem = pl.BlockSpec(memory_space=pltpu.VMEM)
    hbm = pl.BlockSpec(memory_space=pl.ANY)
    shapes = [array.shape for array in arrays[::2]]
    rows = shapes[0][0]
    parts = [(1, width) for _, width in shapes]
    lates = [(count, shapes[which][1]) for which, _, count, late in sorted(pieces, key=lambda p: p[3]) if late > 0]
    which, _, count, _ = [piece for piece in pieces if piece[3] == RAW][0]
    return pl.pallas_call(
        functools.partial(carry_kernel, n_zero, pieces),
        out_shape=(
            *(jax.ShapeDtypeStruct((n_zero * rows, width), jnp.bfloat16) for _, width in shapes),
            *(jax.ShapeDtypeStruct(part, jnp.float32) for part in parts),
            jax.ShapeDtypeStruct((n_zero,) + train.shape, jnp.bfloat16),
            *(jax.ShapeDtypeStruct(shape, jnp.bfloat16) for shape in lates),
        ),
        in_specs=[hbm] * 6 + [vmem] * 3,
        out_specs=(*[hbm] * 3, *[vmem] * 4, *[hbm] * len(lates)),
        scratch_shapes=[
            *(pltpu.VMEM(shape, jnp.float32) for shape in shapes),
            *(pltpu.VMEM(shape, jnp.float32) for shape in shapes),
            *(pltpu.VMEM(shape, jnp.bfloat16) for shape in shapes),
            pltpu.VMEM((rows, LANES), jnp.float32),
            pltpu.VMEM(train.shape, jnp.bfloat16),
            *(pltpu.VMEM((n_zero,) + part, jnp.float32) for part in parts),
            *(pltpu.VMEM(part, jnp.float32) for part in parts),
            *(pltpu.VMEM((2, count, shapes[which][1]), kind) for kind in (jnp.float32, jnp.bfloat16)),
            pltpu.SemaphoreType.DMA((3, 2, CHUNKS)),
            pltpu.SemaphoreType.DMA((len(pieces),)),
            pltpu.SemaphoreType.DMA((LATE,)),
            pltpu.SemaphoreType.DMA((4, n_zero)),
            pltpu.SemaphoreType.DMA((4, n_zero)),
            pltpu.SemaphoreType.DMA,
            pltpu.SemaphoreType.DMA((2, len(pieces))),
            pltpu.SemaphoreType.DMA((2, n_zero, len(pieces))),
            pltpu.SemaphoreType.DMA((3, 2)),
        ],
        compiler_params=pltpu.CompilerParams(
            collective_id=0, has_side_effects=True, vmem_limit_bytes=60 * 2**20
        ),
        name="carry",
    )(*arrays, share, train, step)


def spread_kernel(n_model, part_ref, all_ref, sent, got, own):
    m = lax.axis_index("model")
    barrier = pltpu.get_barrier_semaphore()
    peers = [lax.rem(m + k, n_model) for k in range(1, n_model)]
    for peer in peers:
        pl.semaphore_signal(barrier, inc=1, device_id={"model": peer}, device_id_type=MESH)
    mine = pltpu.make_async_copy(part_ref, all_ref.at[m], own)
    mine.start()
    pl.semaphore_wait(barrier, n_model - 1)
    copies = []
    for k, peer in enumerate(peers, 1):
        copies.append(
            pltpu.make_async_remote_copy(
                src_ref=part_ref,
                dst_ref=all_ref.at[m],
                send_sem=sent.at[k],
                recv_sem=got.at[k],
                device_id={"model": peer},
                device_id_type=MESH,
            )
        )
    for copy in copies:
        copy.start()
    for copy in copies + [mine]:
        copy.wait()


def spread(n_model, part):
    vmem = pl.BlockSpec(memory_space=pltpu.VMEM)
    return pl.pallas_call(
        functools.partial(spread_kernel, n_model),
        out_shape=jax.ShapeDtypeStruct((n_model,) + part.shape, part.dtype),
        in_specs=[vmem],
        out_specs=vmem,
        scratch_shapes=[
            pltpu.SemaphoreType.DMA((n_model,)),
            pltpu.SemaphoreType.DMA((n_model,)),
            pltpu.SemaphoreType.DMA,
        ],
        compiler_params=pltpu.CompilerParams(collective_id=1, has_side_effects=True),
        cost_estimate=pl.CostEstimate(flops=20_000_000, bytes_accessed=65536, transcendentals=0),
        name="spread",
    )(part)


def settle_kernel(plan, *refs):
    sources, targets, spaces = refs[0:3], refs[3:6], refs[6:9]
    read_sem, write_sem = refs[9:]

    def reading(i):
        which, low, count, slot, _ = plan[i]
        return pltpu.make_async_copy(sources[which].at[pl.ds(low, count)], spaces[which].at[slot], read_sem.at[i])

    def writing(i):
        which, low, count, slot, _ = plan[i]
        return pltpu.make_async_copy(spaces[which].at[slot], targets[which].at[pl.ds(low, count)], write_sem.at[i])

    def read_after(i):
        for k, step in enumerate(plan):
            if step[4] == i:
                reading(k).start()

    read_after(None)
    for i in range(len(plan)):
        reading(i).wait()
        writing(i).start()
        if i >= LAG:
            writing(i - LAG).wait()
            read_after(i - LAG)
    for i in range(max(0, len(plan) - LAG), len(plan)):
        writing(i).wait()


def settle(arrays):
    plan, spaces = [], []
    for which in (1, 2, 0):
        step = arrays[which].shape[0] // COPIES[which]
        first = len(plan)
        for k in range(COPIES[which]):
            after = first + k - SLOTS[which] if k >= SLOTS[which] else None
            plan.append((which, k * step, step, k % SLOTS[which], after))
    for which, array in enumerate(arrays):
        step = array.shape[0] // COPIES[which]
        spaces.append(pltpu.VMEM((SLOTS[which], step, array.shape[1]), array.dtype))
    hbm = pl.BlockSpec(memory_space=pl.ANY)
    size = sum(array.shape[0] * array.shape[1] for array in arrays)
    return pl.pallas_call(
        functools.partial(settle_kernel, tuple(plan)),
        out_shape=tuple(jax.ShapeDtypeStruct(array.shape, array.dtype) for array in arrays),
        in_specs=[hbm] * 3,
        out_specs=(hbm,) * 3,
        scratch_shapes=spaces
        + [pltpu.SemaphoreType.DMA((len(plan),)), pltpu.SemaphoreType.DMA((len(plan),))],
        compiler_params=pltpu.CompilerParams(vmem_limit_bytes=40 * 2**20),
        cost_estimate=pl.CostEstimate(flops=8 * size, bytes_accessed=4 * size, transcendentals=0),
        name="settle",
    )(*arrays)


def on_device(n_zero, n_model, *args):
    arrays = args[:6]
    mix_share, norm_train, norm_step = args[6:]
    rows = mix_share.shape[0]
    z, unit = lax.axis_index("zero"), lax.axis_index("unit")
    edges = (0, 3 * rows // 32, rows // 4, rows)
    pieces = [(1, low, high - low, late) for low, high, late in zip(edges, edges[1:], (RAW, 0, 0))]
    pieces.append((2, 0, rows, 0))
    bounds = [cut * rows // CUTS[-1] for cut in CUTS]
    for k, late in enumerate(LATES):
        pieces.append((0, bounds[k], bounds[k + 1] - bounds[k], late))
    results = carry(
        n_zero,
        tuple(pieces),
        arrays,
        mix_share.reshape(-1, LANES),
        norm_train[None, :],
        norm_step[None, :],
    )
    serve, totals, gain, lates = list(results[:3]), results[3:6], results[6], results[7:]
    swap = [(k, k ^ 1) for k in range(n_zero)]
    partner = z + 1 - 2 * lax.rem(z, 2)
    landed = serve[0]
    serve = list(settle(serve))
    for late in range(1, LATE + 1):
        _, low, count, _ = pieces[LATES.index(late) - len(LATES)]
        where = (partner * rows + low, jnp.zeros_like(z))
        if late != STAGGER:
            block = lax.ppermute(lates[late - 1], "zero", swap)
        else:
            block = lax.ppermute(lates[late - 1], ("unit", "zero"), swap)
            there = lax.dynamic_slice(landed, where, (count, landed.shape[1]))
            block = jnp.where(unit == 0, block, there)
        serve[0] = lax.dynamic_update_slice(serve[0], block, where)
    totals, gain, _ = lax.optimization_barrier((totals, gain, serve[1]))
    factors = [jnp.sqrt(total[0]) for total in totals]
    gain = spread(n_model, gain)
    gain = gain.reshape(n_model, n_zero, -1).transpose(1, 0, 2)
    return (*serve, *factors, gain.reshape(-1))


def solution(mesh):
    in_specs = (
        P(("unit", "zero"), "model"),
        P(("unit", "zero"), "model"),
        P(("unit", "zero"), "model"),
        P(("unit", "zero"), "model"),
        P(("unit", "zero"), "model"),
        P(("unit", "zero"), "model"),
        P(("unit", "zero")),
        P(("unit", "zero", "model")),
        P(("unit", "zero", "model")),
    )
    out_specs = (
        P("unit", "model"),
        P("unit", "model"),
        P("unit", "model"),
        P(("unit", "model")),
        P(("unit", "model")),
        P(("unit", "model")),
        P("unit"),
    )
    return jax.shard_map(
        functools.partial(on_device, mesh.shape["zero"], mesh.shape["model"]),
        mesh=mesh,
        in_specs=in_specs,
        out_specs=out_specs,
        check_vma=False,
    )
```

```python
import functools
import math

import jax
import jax.numpy as jnp
from jax import lax
from jax.experimental import pallas as pl
from jax.experimental.pallas import tpu as pltpu
from jax.sharding import PartitionSpec as P

MESH = pl.DeviceIdType.MESH
LANES = 128
GROUP = 32
EARLY = 8
CHUNKS = 16
HEAD = 3
CUTS = (0, 8, 16, 20, 24, 31, 32)
LATES = (0, 0, 0, 2, 1, 3)
LATE = 3
STAGGER = 2
RAW = -1
COPIES = (16, 4, 4)
SLOTS = (8, 4, 4)
LAG = 4


def total_of(held, n_zero):
    total = held[0]
    for k in range(1, n_zero):
        total = total + held[k]
    return total


def slabs_of(width):
    return [(low, min(LANES, width - low)) for low in range(0, width, LANES)]


def mix_rows(first, second, wide, low, count, sums):
    group = math.gcd(GROUP, count)
    slabs = slabs_of(first.shape[1])

    def step(i, sums):
        here = pl.ds(pl.multiple_of(low + i * group, group), group)
        share = wide[here, :]
        rest = 1.0 - share
        out = []
        for (start, size), total in zip(slabs, sums):
            columns = pl.ds(start, size)
            fresh = share[:, :size] * first[here, columns] + rest[:, :size] * second[here, columns]
            first[here, columns] = fresh
            out.append(total + jnp.sum((fresh * fresh).reshape(group // 8, 8, size), axis=0))
        return tuple(out)

    return lax.fori_loop(0, count // group, step, tuple(sums))


def narrow_rows(fresh, own, scale, low, count):
    group = math.gcd(GROUP, count)
    slabs = slabs_of(fresh.shape[1])
    scales = [jnp.broadcast_to(scale[:, start : start + size], (group, size)) for start, size in slabs]

    def step(i, carry):
        here = pl.ds(pl.multiple_of(low + i * group, group), group)
        for (start, size), factor in zip(slabs, scales):
            columns = pl.ds(start, size)
            own[here, columns] = (fresh[here, columns] * factor).astype(own.dtype)
        return carry

    lax.fori_loop(0, count // group, step, 0)


def carry_kernel(n_zero, pieces, *refs):
    inputs, outputs, scratch = refs[:9], refs[9 : 16 + LATE], refs[16 + LATE :]
    sources = (inputs[0:2], inputs[2:4], inputs[4:6])
    share_ref, train_ref, step_ref = inputs[6:]
    serve, totals, gain_ref = outputs[0:3], outputs[3:6], outputs[6]
    late_refs = outputs[7:]
    fresh, second, own = scratch[0:3], scratch[3:6], scratch[6:9]
    wide, norm = scratch[9:11]
    held, part = scratch[11:14], scratch[14:17]
    raw_held, raw_own = scratch[17:19]
    read_sem, own_sem, late_sem, stat_sent, stat_got, norm_sem, sent, got, raw_sem = scratch[19:]

    z = lax.axis_index("zero")
    lead_unit = lax.axis_index("unit") == 0
    rows = fresh[0].shape[0]
    barrier = pltpu.get_barrier_semaphore()
    peers = [lax.rem(z + k, n_zero) for k in range(1, n_zero)]
    for peer in peers:
        pl.semaphore_signal(barrier, inc=1, device_id={"zero": peer}, device_id_type=MESH)

    def read(which, k, chunks):
        step = rows // chunks
        here = pl.ds(k * step, step)
        return [
            pltpu.make_async_copy(source.at[here], target.at[here], read_sem.at[which, side, k])
            for side, (source, target) in enumerate(zip(sources[which], (fresh[which], second[which])))
        ]

    def start(copies):
        for copy in copies:
            copy.start()

    def finish(copies):
        for copy in copies:
            copy.wait()

    for k in range(EARLY):
        start(read(1, k, EARLY))
    norm[...] = (train_ref[...] + step_ref[...]).astype(norm.dtype)
    for k in range(rows // LANES):
        line = jnp.broadcast_to(share_ref[k : k + 1, :], (LANES, LANES))
        wide[k * LANES : (k + 1) * LANES, :] = jnp.transpose(line)

    def sums_start(which):
        return tuple(jnp.zeros((8, size), jnp.float32) for _, size in slabs_of(fresh[which].shape[1]))

    def tally(which, sums, low, high, chunks):
        step = rows // chunks
        for k in range(low, high):
            finish(read(which, k, chunks))
            sums = mix_rows(fresh[which], second[which], wide, k * step, step, sums)
        return sums

    def close(which, sums):
        for (start_at, size), value in zip(slabs_of(fresh[which].shape[1]), sums):
            part[which][:, start_at : start_at + size] = jnp.sum(value, axis=0, keepdims=True)

    def exchange(index, source, target):
        copies = []
        for k, peer in enumerate(peers, 1):
            copies.append(
                pltpu.make_async_remote_copy(
                    src_ref=source,
                    dst_ref=target.at[z],
                    send_sem=stat_sent.at[index, k],
                    recv_sem=stat_got.at[index, k],
                    device_id={"zero": peer},
                    device_id_type=MESH,
                )
            )
        start(copies)
        return copies

    def move(p, hop, way, owner, source=None):
        which, low, count, _ = pieces[p]
        here = pl.ds(pl.multiple_of(owner * rows + low, 8), count)
        target = serve[which].at[here]
        return pltpu.make_async_remote_copy(
            src_ref=target if source is None else source,
            dst_ref=target,
            send_sem=sent.at[way, p],
            recv_sem=got.at[way, hop, p],
            device_id={"zero": lax.rem(z + (1 if way == 0 else n_zero - 1), n_zero)},
            device_id_type=MESH,
        )

    ranks = (z, n_zero - 1 - z)

    def kept(p, hop, rank, last):
        skip = jnp.logical_and(hop == 0, rank == last)
        if pieces[p][3] == STAGGER:
            skip = jnp.logical_and(skip, lead_unit)
        return jnp.logical_not(skip)

    def sends(p, hop, way):
        rank = ranks[way]
        yes = jnp.logical_and(rank < n_zero - 1, rank >= hop)
        if pieces[p][3] == RAW:
            yes = jnp.logical_and(yes, hop >= 1)
        elif pieces[p][3]:
            yes = jnp.logical_and(yes, kept(p, hop, rank, n_zero - 2))
        return yes

    def arrives(p, hop, way):
        rank = ranks[way]
        yes = rank >= hop + 1
        if pieces[p][3] == RAW:
            yes = jnp.logical_and(yes, hop >= 1)
        elif pieces[p][3]:
            yes = jnp.logical_and(yes, kept(p, hop, rank, n_zero - 1))
        return yes

    def own_copies(p):
        which, low, count, late = pieces[p]
        source = own[which].at[pl.ds(low, count)]
        here = pl.ds(pl.multiple_of(z * rows + low, 8), count)
        copies = [pltpu.make_async_copy(source, serve[which].at[here], own_sem.at[p])]
        if late > 0:
            copies.append(pltpu.make_async_copy(source, late_refs[late - 1], late_sem.at[late - 1]))
        return copies

    def first_move(p, way):
        which, low, count, _ = pieces[p]
        return move(p, 0, way, z, own[which].at[pl.ds(low, count)])

    def launch(p):
        if pieces[p][3] != RAW:
            for way in (0, 1):

                @pl.when(sends(p, 0, way))
                def _():
                    first_move(p, way).start()

        start(own_copies(p))

    raw = [p for p, piece in enumerate(pieces) if piece[3] == RAW][0]
    raw_which, raw_low, raw_count, _ = pieces[raw]

    def raw_move(way):
        return pltpu.make_async_remote_copy(
            src_ref=fresh[raw_which].at[pl.ds(raw_low, raw_count)],
            dst_ref=raw_held.at[way],
            send_sem=raw_sem.at[0, way],
            recv_sem=raw_sem.at[1, way],
            device_id={"zero": lax.rem(z + (1 if way == 0 else n_zero - 1), n_zero)},
            device_id_type=MESH,
        )

    def raw_copy(way):
        owner = lax.rem(z + (n_zero - 1 if way == 0 else 1), n_zero)
        here = pl.ds(pl.multiple_of(owner * rows + raw_low, 8), raw_count)
        return pltpu.make_async_copy(raw_own.at[way], serve[raw_which].at[here], raw_sem.at[2, way])

    def settle(which, copies):
        finish(copies)
        total = total_of(held[which], n_zero)
        totals[which][...] = total
        return 1.0 / jnp.sqrt(total)

    def send_own(which, scale):
        for p, (owner, low, count, late) in sorted(enumerate(pieces), key=lambda item: item[1][3] == RAW):
            if owner == which:
                narrow_rows(fresh[which], own[which], scale, low, count)
                launch(p)

    sums = tally(1, sums_start(1), 0, EARLY // 2, EARLY)
    for k in range(EARLY):
        start(read(2, k, EARLY))
    sums = tally(1, sums, EARLY // 2, EARLY, EARLY)
    close(1, sums)
    for k in range(CHUNKS):
        start(read(0, k, CHUNKS))
    held[1][z] = part[1][...]
    pl.semaphore_wait(barrier, n_zero - 1)
    key_copies = exchange(1, part[1], held[1])
    for way in (0, 1):

        @pl.when(ranks[way] < n_zero - 1)
        def _():
            raw_move(way).start()

    sums = tally(2, sums_start(2), 0, EARLY, EARLY)
    close(2, sums)
    held[2][z] = part[2][...]
    value_copies = exchange(2, part[2], held[2])
    norm_copies = exchange(3, norm, gain_ref)
    norm_copies.append(pltpu.make_async_copy(norm, gain_ref.at[z], norm_sem))
    norm_copies[-1].start()
    sums = tally(0, sums_start(0), 0, HEAD, CHUNKS)
    scale = settle(1, key_copies)
    send_own(1, scale)
    for way in (0, 1):

        @pl.when(ranks[way] >= 1)
        def _():
            raw_move(way).wait_recv()
            narrow_rows(raw_held.at[way], raw_own.at[way], scale, 0, raw_count)
            raw_copy(way).start()

    sums = tally(0, sums, HEAD, CHUNKS, CHUNKS)
    close(0, sums)
    held[0][z] = part[0][...]
    query_copies = exchange(0, part[0], held[0])
    scale = settle(2, value_copies)
    send_own(2, scale)
    scale = settle(0, query_copies)
    send_own(0, scale)

    def relay(hop, carry):
        for p in range(len(pieces)):
            for way in (0, 1):
                owner = lax.rem(z + (n_zero - hop if way == 0 else hop), n_zero)
                before = lax.rem(z + (n_zero - hop + 1 if way == 0 else hop - 1), n_zero)

                @pl.when(arrives(p, hop - 1, way))
                def _():
                    move(p, hop - 1, way, owner).wait_recv()

                @pl.when(sends(p, hop, way))
                def _():
                    @pl.when(sends(p, hop - 1, way))
                    def _():
                        move(p, hop - 1, way, before).wait_send()

                    move(p, hop, way, owner).start()

        return carry

    for way in (0, 1):

        @pl.when(ranks[way] >= 1)
        def _():
            raw_copy(way).wait()

        @pl.when(ranks[way] < n_zero - 1)
        def _():
            raw_move(way).wait_send()

    lax.fori_loop(1, n_zero, relay, 0)
    for p in range(len(pieces)):
        for way in (0, 1):
            rank = ranks[way]

            @pl.when(sends(p, rank, way))
            def _():
                move(p, 0, way, z).wait_send()

    for p in range(len(pieces)):
        finish(own_copies(p))
    finish(norm_copies)


def carry(n_zero, pieces, arrays, share, train, step):
    vmem = pl.BlockSpec(memory_space=pltpu.VMEM)
    hbm = pl.BlockSpec(memory_space=pl.ANY)
    shapes = [array.shape for array in arrays[::2]]
    rows = shapes[0][0]
    parts = [(1, width) for _, width in shapes]
    lates = [(count, shapes[which][1]) for which, _, count, late in sorted(pieces, key=lambda p: p[3]) if late > 0]
    which, _, count, _ = [piece for piece in pieces if piece[3] == RAW][0]
    return pl.pallas_call(
        functools.partial(carry_kernel, n_zero, pieces),
        out_shape=(
            *(jax.ShapeDtypeStruct((n_zero * rows, width), jnp.bfloat16) for _, width in shapes),
            *(jax.ShapeDtypeStruct(part, jnp.float32) for part in parts),
            jax.ShapeDtypeStruct((n_zero,) + train.shape, jnp.bfloat16),
            *(jax.ShapeDtypeStruct(shape, jnp.bfloat16) for shape in lates),
        ),
        in_specs=[hbm] * 6 + [vmem] * 3,
        out_specs=(*[hbm] * 3, *[vmem] * 4, *[hbm] * len(lates)),
        scratch_shapes=[
            *(pltpu.VMEM(shape, jnp.float32) for shape in shapes),
            *(pltpu.VMEM(shape, jnp.float32) for shape in shapes),
            *(pltpu.VMEM(shape, jnp.bfloat16) for shape in shapes),
            pltpu.VMEM((rows, LANES), jnp.float32),
            pltpu.VMEM(train.shape, jnp.bfloat16),
            *(pltpu.VMEM((n_zero,) + part, jnp.float32) for part in parts),
            *(pltpu.VMEM(part, jnp.float32) for part in parts),
            *(pltpu.VMEM((2, count, shapes[which][1]), kind) for kind in (jnp.float32, jnp.bfloat16)),
            pltpu.SemaphoreType.DMA((3, 2, CHUNKS)),
            pltpu.SemaphoreType.DMA((len(pieces),)),
            pltpu.SemaphoreType.DMA((LATE,)),
            pltpu.SemaphoreType.DMA((4, n_zero)),
            pltpu.SemaphoreType.DMA((4, n_zero)),
            pltpu.SemaphoreType.DMA,
            pltpu.SemaphoreType.DMA((2, len(pieces))),
            pltpu.SemaphoreType.DMA((2, n_zero, len(pieces))),
            pltpu.SemaphoreType.DMA((3, 2)),
        ],
        compiler_params=pltpu.CompilerParams(
            collective_id=0, has_side_effects=True, vmem_limit_bytes=60 * 2**20
        ),
        name="carry",
    )(*arrays, share, train, step)


def spread_kernel(n_model, part_ref, all_ref, sent, got, own):
    m = lax.axis_index("model")
    barrier = pltpu.get_barrier_semaphore()
    peers = [lax.rem(m + k, n_model) for k in range(1, n_model)]
    for peer in peers:
        pl.semaphore_signal(barrier, inc=1, device_id={"model": peer}, device_id_type=MESH)
    mine = pltpu.make_async_copy(part_ref, all_ref.at[m], own)
    mine.start()
    pl.semaphore_wait(barrier, n_model - 1)
    copies = []
    for k, peer in enumerate(peers, 1):
        copies.append(
            pltpu.make_async_remote_copy(
                src_ref=part_ref,
                dst_ref=all_ref.at[m],
                send_sem=sent.at[k],
                recv_sem=got.at[k],
                device_id={"model": peer},
                device_id_type=MESH,
            )
        )
    for copy in copies:
        copy.start()
    for copy in copies + [mine]:
        copy.wait()


def spread(n_model, part):
    vmem = pl.BlockSpec(memory_space=pltpu.VMEM)
    return pl.pallas_call(
        functools.partial(spread_kernel, n_model),
        out_shape=jax.ShapeDtypeStruct((n_model,) + part.shape, part.dtype),
        in_specs=[vmem],
        out_specs=vmem,
        scratch_shapes=[
            pltpu.SemaphoreType.DMA((n_model,)),
            pltpu.SemaphoreType.DMA((n_model,)),
            pltpu.SemaphoreType.DMA,
        ],
        compiler_params=pltpu.CompilerParams(collective_id=1, has_side_effects=True),
        cost_estimate=pl.CostEstimate(flops=20_000_000, bytes_accessed=65536, transcendentals=0),
        name="spread",
    )(part)


def settle_kernel(plan, *refs):
    sources, targets, spaces = refs[0:3], refs[3:6], refs[6:9]
    read_sem, write_sem = refs[9:]

    def reading(i):
        which, low, count, slot, _ = plan[i]
        return pltpu.make_async_copy(sources[which].at[pl.ds(low, count)], spaces[which].at[slot], read_sem.at[i])

    def writing(i):
        which, low, count, slot, _ = plan[i]
        return pltpu.make_async_copy(spaces[which].at[slot], targets[which].at[pl.ds(low, count)], write_sem.at[i])

    def read_after(i):
        for k, step in enumerate(plan):
            if step[4] == i:
                reading(k).start()

    read_after(None)
    for i in range(len(plan)):
        reading(i).wait()
        writing(i).start()
        if i >= LAG:
            writing(i - LAG).wait()
            read_after(i - LAG)
    for i in range(max(0, len(plan) - LAG), len(plan)):
        writing(i).wait()


def settle(arrays):
    plan, spaces = [], []
    for which in (1, 2, 0):
        step = arrays[which].shape[0] // COPIES[which]
        first = len(plan)
        for k in range(COPIES[which]):
            after = first + k - SLOTS[which] if k >= SLOTS[which] else None
            plan.append((which, k * step, step, k % SLOTS[which], after))
    for which, array in enumerate(arrays):
        step = array.shape[0] // COPIES[which]
        spaces.append(pltpu.VMEM((SLOTS[which], step, array.shape[1]), array.dtype))
    hbm = pl.BlockSpec(memory_space=pl.ANY)
    size = sum(array.shape[0] * array.shape[1] for array in arrays)
    return pl.pallas_call(
        functools.partial(settle_kernel, tuple(plan)),
        out_shape=tuple(jax.ShapeDtypeStruct(array.shape, array.dtype) for array in arrays),
        in_specs=[hbm] * 3,
        out_specs=(hbm,) * 3,
        scratch_shapes=spaces
        + [pltpu.SemaphoreType.DMA((len(plan),)), pltpu.SemaphoreType.DMA((len(plan),))],
        compiler_params=pltpu.CompilerParams(vmem_limit_bytes=40 * 2**20),
        cost_estimate=pl.CostEstimate(flops=8 * size, bytes_accessed=4 * size, transcendentals=0),
        name="settle",
    )(*arrays)


def on_device(n_zero, n_model, *args):
    arrays = args[:6]
    mix_share, norm_train, norm_step = args[6:]
    rows = mix_share.shape[0]
    z, unit = lax.axis_index("zero"), lax.axis_index("unit")
    edges = (0, 3 * rows // 32, rows // 4, rows)
    pieces = [(1, low, high - low, late) for low, high, late in zip(edges, edges[1:], (RAW, 0, 0))]
    pieces.append((2, 0, rows, 0))
    bounds = [cut * rows // CUTS[-1] for cut in CUTS]
    for k, late in enumerate(LATES):
        pieces.append((0, bounds[k], bounds[k + 1] - bounds[k], late))
    results = carry(
        n_zero,
        tuple(pieces),
        arrays,
        mix_share.reshape(-1, LANES),
        norm_train[None, :],
        norm_step[None, :],
    )
    serve, totals, gain, lates = list(results[:3]), results[3:6], results[6], results[7:]
    swap = [(k, k ^ 1) for k in range(n_zero)]
    partner = z + 1 - 2 * lax.rem(z, 2)
    landed = serve[0]
    serve = list(settle(serve))
    for late in range(1, LATE + 1):
        _, low, count, _ = pieces[LATES.index(late) - len(LATES)]
        where = (partner * rows + low, jnp.zeros_like(z))
        if late != STAGGER:
            block = lax.ppermute(lates[late - 1], "zero", swap)
        else:
            block = lax.ppermute(lates[late - 1], ("unit", "zero"), swap)
            there = lax.dynamic_slice(landed, where, (count, landed.shape[1]))
            block = jnp.where(unit == 0, block, there)
        serve[0] = lax.dynamic_update_slice(serve[0], block, where)
    totals, gain, _ = lax.optimization_barrier((totals, gain, serve[1]))
    factors = [jnp.sqrt(total[0]) for total in totals]
    gain = spread(n_model, gain)
    gain = gain.reshape(n_model, n_zero, -1).transpose(1, 0, 2)
    return (*serve, *factors, gain.reshape(-1))


def solution(mesh):
    in_specs = (
        P(("unit", "zero"), "model"),
        P(("unit", "zero"), "model"),
        P(("unit", "zero"), "model"),
        P(("unit", "zero"), "model"),
        P(("unit", "zero"), "model"),
        P(("unit", "zero"), "model"),
        P(("unit", "zero")),
        P(("unit", "zero", "model")),
        P(("unit", "zero", "model")),
    )
    out_specs = (
        P("unit", "model"),
        P("unit", "model"),
        P("unit", "model"),
        P(("unit", "model")),
        P(("unit", "model")),
        P(("unit", "model")),
        P("unit"),
    )
    return jax.shard_map(
        functools.partial(on_device, mesh.shape["zero"], mesh.shape["model"]),
        mesh=mesh,
        in_specs=in_specs,
        out_specs=out_specs,
        check_vma=False,
    )
```

```python
import functools
import math

import jax
import jax.numpy as jnp
from jax import lax
from jax.experimental import pallas as pl
from jax.experimental.pallas import tpu as pltpu
from jax.sharding import PartitionSpec as P

MESH = pl.DeviceIdType.MESH
LANES = 128
GROUP = 32
WORDS = 2**15
EARLY = 8
CHUNKS = 16
HEAD = 3
CUTS = (0, 8, 16, 20, 24, 31, 32)
LATES = (0, 0, 0, 2, 1, 3)
LATE = 3
STAGGER = 2
RAW = -1
COPIES = (16, 4, 4)
SLOTS = (8, 4, 4)
LAG = 4


def total_of(held, n_zero):
    total = held[0]
    for k in range(1, n_zero):
        total = total + held[k]
    return total


def slabs_of(width):
    return [(low, min(LANES, width - low)) for low in range(0, width, LANES)]


def mix_rows(first, second, wide, low, count, sums):
    group = math.gcd(max(GROUP, WORDS // first.shape[1]), count)
    slabs = slabs_of(first.shape[1])

    def step(i, sums):
        here = pl.ds(pl.multiple_of(low + i * group, group), group)
        share = wide[here, :]
        rest = 1.0 - share
        out = []
        for (start, size), total in zip(slabs, sums):
            columns = pl.ds(start, size)
            fresh = share[:, :size] * first[here, columns] + rest[:, :size] * second[here, columns]
            first[here, columns] = fresh
            out.append(total + jnp.sum((fresh * fresh).reshape(group // 8, 8, size), axis=0))
        return tuple(out)

    return lax.fori_loop(0, count // group, step, tuple(sums))


def narrow_rows(fresh, own, scale, low, count):
    group = math.gcd(max(GROUP, WORDS // fresh.shape[1]), count)
    slabs = slabs_of(fresh.shape[1])
    scales = [jnp.broadcast_to(scale[:, start : start + size], (group, size)) for start, size in slabs]

    def step(i, carry):
        here = pl.ds(pl.multiple_of(low + i * group, group), group)
        for (start, size), factor in zip(slabs, scales):
            columns = pl.ds(start, size)
            own[here, columns] = (fresh[here, columns] * factor).astype(own.dtype)
        return carry

    lax.fori_loop(0, count // group, step, 0)


def carry_kernel(n_zero, pieces, *refs):
    inputs, outputs, scratch = refs[:9], refs[9 : 16 + LATE], refs[16 + LATE :]
    sources = (inputs[0:2], inputs[2:4], inputs[4:6])
    share_ref, train_ref, step_ref = inputs[6:]
    serve, totals, gain_ref = outputs[0:3], outputs[3:6], outputs[6]
    late_refs = outputs[7:]
    fresh, second, own = scratch[0:3], scratch[3:6], scratch[6:9]
    wide, norm = scratch[9:11]
    held, part = scratch[11:14], scratch[14:17]
    raw_held, raw_own = scratch[17:19]
    read_sem, own_sem, late_sem, stat_sent, stat_got, norm_sem, sent, got, raw_sem = scratch[19:]

    z = lax.axis_index("zero")
    lead_unit = lax.axis_index("unit") == 0
    rows = fresh[0].shape[0]
    barrier = pltpu.get_barrier_semaphore()
    peers = [lax.rem(z + k, n_zero) for k in range(1, n_zero)]
    for peer in peers:
        pl.semaphore_signal(barrier, inc=1, device_id={"zero": peer}, device_id_type=MESH)

    def read(which, k, chunks):
        step = rows // chunks
        here = pl.ds(k * step, step)
        return [
            pltpu.make_async_copy(source.at[here], target.at[here], read_sem.at[which, side, k])
            for side, (source, target) in enumerate(zip(sources[which], (fresh[which], second[which])))
        ]

    def start(copies):
        for copy in copies:
            copy.start()

    def finish(copies):
        for copy in copies:
            copy.wait()

    for k in range(EARLY):
        start(read(1, k, EARLY))
    norm[...] = (train_ref[...] + step_ref[...]).astype(norm.dtype)
    for k in range(rows // LANES):
        line = jnp.broadcast_to(share_ref[k : k + 1, :], (LANES, LANES))
        wide[k * LANES : (k + 1) * LANES, :] = jnp.transpose(line)

    def sums_start(which):
        return tuple(jnp.zeros((8, size), jnp.float32) for _, size in slabs_of(fresh[which].shape[1]))

    def tally(which, sums, low, high, chunks):
        step = rows // chunks
        for k in range(low, high):
            finish(read(which, k, chunks))
            sums = mix_rows(fresh[which], second[which], wide, k * step, step, sums)
        return sums

    def close(which, sums):
        for (start_at, size), value in zip(slabs_of(fresh[which].shape[1]), sums):
            part[which][:, start_at : start_at + size] = jnp.sum(value, axis=0, keepdims=True)

    def exchange(index, source, target):
        copies = []
        for k, peer in enumerate(peers, 1):
            copies.append(
                pltpu.make_async_remote_copy(
                    src_ref=source,
                    dst_ref=target.at[z],
                    send_sem=stat_sent.at[index, k],
                    recv_sem=stat_got.at[index, k],
                    device_id={"zero": peer},
                    device_id_type=MESH,
                )
            )
        start(copies)
        return copies

    def move(p, hop, way, owner, source=None):
        which, low, count, _ = pieces[p]
        here = pl.ds(pl.multiple_of(owner * rows + low, 8), count)
        target = serve[which].at[here]
        return pltpu.make_async_remote_copy(
            src_ref=target if source is None else source,
            dst_ref=target,
            send_sem=sent.at[way, p],
            recv_sem=got.at[way, hop, p],
            device_id={"zero": lax.rem(z + (1 if way == 0 else n_zero - 1), n_zero)},
            device_id_type=MESH,
        )

    ranks = (z, n_zero - 1 - z)

    def kept(p, hop, rank, last):
        skip = jnp.logical_and(hop == 0, rank == last)
        if pieces[p][3] == STAGGER:
            skip = jnp.logical_and(skip, lead_unit)
        return jnp.logical_not(skip)

    def sends(p, hop, way):
        rank = ranks[way]
        yes = jnp.logical_and(rank < n_zero - 1, rank >= hop)
        if pieces[p][3] == RAW:
            yes = jnp.logical_and(yes, hop >= 1)
        elif pieces[p][3]:
            yes = jnp.logical_and(yes, kept(p, hop, rank, n_zero - 2))
        return yes

    def arrives(p, hop, way):
        rank = ranks[way]
        yes = rank >= hop + 1
        if pieces[p][3] == RAW:
            yes = jnp.logical_and(yes, hop >= 1)
        elif pieces[p][3]:
            yes = jnp.logical_and(yes, kept(p, hop, rank, n_zero - 1))
        return yes

    def own_copies(p):
        which, low, count, late = pieces[p]
        source = own[which].at[pl.ds(low, count)]
        here = pl.ds(pl.multiple_of(z * rows + low, 8), count)
        copies = [pltpu.make_async_copy(source, serve[which].at[here], own_sem.at[p])]
        if late > 0:
            copies.append(pltpu.make_async_copy(source, late_refs[late - 1], late_sem.at[late - 1]))
        return copies

    def first_move(p, way):
        which, low, count, _ = pieces[p]
        return move(p, 0, way, z, own[which].at[pl.ds(low, count)])

    def launch(p):
        if pieces[p][3] != RAW:
            for way in (0, 1):

                @pl.when(sends(p, 0, way))
                def _():
                    first_move(p, way).start()

        start(own_copies(p))

    raw = [p for p, piece in enumerate(pieces) if piece[3] == RAW][0]
    raw_which, raw_low, raw_count, _ = pieces[raw]

    def raw_move(way):
        return pltpu.make_async_remote_copy(
            src_ref=fresh[raw_which].at[pl.ds(raw_low, raw_count)],
            dst_ref=raw_held.at[way],
            send_sem=raw_sem.at[0, way],
            recv_sem=raw_sem.at[1, way],
            device_id={"zero": lax.rem(z + (1 if way == 0 else n_zero - 1), n_zero)},
            device_id_type=MESH,
        )

    def raw_copy(way):
        owner = lax.rem(z + (n_zero - 1 if way == 0 else 1), n_zero)
        here = pl.ds(pl.multiple_of(owner * rows + raw_low, 8), raw_count)
        return pltpu.make_async_copy(raw_own.at[way], serve[raw_which].at[here], raw_sem.at[2, way])

    def settle(which, copies):
        finish(copies)
        total = total_of(held[which], n_zero)
        totals[which][...] = total
        return 1.0 / jnp.sqrt(total)

    def send_own(which, scale):
        for p, (owner, low, count, late) in sorted(enumerate(pieces), key=lambda item: item[1][3] == RAW):
            if owner == which:
                narrow_rows(fresh[which], own[which], scale, low, count)
                launch(p)

    sums = tally(1, sums_start(1), 0, EARLY // 2, EARLY)
    for k in range(EARLY):
        start(read(2, k, EARLY))
    sums = tally(1, sums, EARLY // 2, EARLY, EARLY)
    close(1, sums)
    for k in range(CHUNKS):
        start(read(0, k, CHUNKS))
    held[1][z] = part[1][...]
    pl.semaphore_wait(barrier, n_zero - 1)
    key_copies = exchange(1, part[1], held[1])
    for way in (0, 1):

        @pl.when(ranks[way] < n_zero - 1)
        def _():
            raw_move(way).start()

    sums = tally(2, sums_start(2), 0, EARLY, EARLY)
    close(2, sums)
    held[2][z] = part[2][...]
    value_copies = exchange(2, part[2], held[2])
    norm_copies = exchange(3, norm, gain_ref)
    norm_copies.append(pltpu.make_async_copy(norm, gain_ref.at[z], norm_sem))
    norm_copies[-1].start()
    sums = tally(0, sums_start(0), 0, HEAD, CHUNKS)
    scale = settle(1, key_copies)
    send_own(1, scale)
    for way in (0, 1):

        @pl.when(ranks[way] >= 1)
        def _():
            raw_move(way).wait_recv()
            narrow_rows(raw_held.at[way], raw_own.at[way], scale, 0, raw_count)
            raw_copy(way).start()

    sums = tally(0, sums, HEAD, CHUNKS, CHUNKS)
    close(0, sums)
    held[0][z] = part[0][...]
    query_copies = exchange(0, part[0], held[0])
    scale = settle(2, value_copies)
    send_own(2, scale)
    scale = settle(0, query_copies)
    send_own(0, scale)

    def relay(hop, carry):
        for p in range(len(pieces)):
            for way in (0, 1):
                owner = lax.rem(z + (n_zero - hop if way == 0 else hop), n_zero)
                before = lax.rem(z + (n_zero - hop + 1 if way == 0 else hop - 1), n_zero)

                @pl.when(arrives(p, hop - 1, way))
                def _():
                    move(p, hop - 1, way, owner).wait_recv()

                @pl.when(sends(p, hop, way))
                def _():
                    @pl.when(sends(p, hop - 1, way))
                    def _():
                        move(p, hop - 1, way, before).wait_send()

                    move(p, hop, way, owner).start()

        return carry

    for way in (0, 1):

        @pl.when(ranks[way] >= 1)
        def _():
            raw_copy(way).wait()

        @pl.when(ranks[way] < n_zero - 1)
        def _():
            raw_move(way).wait_send()

    lax.fori_loop(1, n_zero, relay, 0)
    for p in range(len(pieces)):
        for way in (0, 1):
            rank = ranks[way]

            @pl.when(sends(p, rank, way))
            def _():
                move(p, 0, way, z).wait_send()

    for p in range(len(pieces)):
        finish(own_copies(p))
    finish(norm_copies)


def carry(n_zero, pieces, arrays, share, train, step):
    vmem = pl.BlockSpec(memory_space=pltpu.VMEM)
    hbm = pl.BlockSpec(memory_space=pl.ANY)
    shapes = [array.shape for array in arrays[::2]]
    rows = shapes[0][0]
    parts = [(1, width) for _, width in shapes]
    lates = [(count, shapes[which][1]) for which, _, count, late in sorted(pieces, key=lambda p: p[3]) if late > 0]
    which, _, count, _ = [piece for piece in pieces if piece[3] == RAW][0]
    return pl.pallas_call(
        functools.partial(carry_kernel, n_zero, pieces),
        out_shape=(
            *(jax.ShapeDtypeStruct((n_zero * rows, width), jnp.bfloat16) for _, width in shapes),
            *(jax.ShapeDtypeStruct(part, jnp.float32) for part in parts),
            jax.ShapeDtypeStruct((n_zero,) + train.shape, jnp.bfloat16),
            *(jax.ShapeDtypeStruct(shape, jnp.bfloat16) for shape in lates),
        ),
        in_specs=[hbm] * 6 + [vmem] * 3,
        out_specs=(*[hbm] * 3, *[vmem] * 4, *[hbm] * len(lates)),
        scratch_shapes=[
            *(pltpu.VMEM(shape, jnp.float32) for shape in shapes),
            *(pltpu.VMEM(shape, jnp.float32) for shape in shapes),
            *(pltpu.VMEM(shape, jnp.bfloat16) for shape in shapes),
            pltpu.VMEM((rows, LANES), jnp.float32),
            pltpu.VMEM(train.shape, jnp.bfloat16),
            *(pltpu.VMEM((n_zero,) + part, jnp.float32) for part in parts),
            *(pltpu.VMEM(part, jnp.float32) for part in parts),
            *(pltpu.VMEM((2, count, shapes[which][1]), kind) for kind in (jnp.float32, jnp.bfloat16)),
            pltpu.SemaphoreType.DMA((3, 2, CHUNKS)),
            pltpu.SemaphoreType.DMA((len(pieces),)),
            pltpu.SemaphoreType.DMA((LATE,)),
            pltpu.SemaphoreType.DMA((4, n_zero)),
            pltpu.SemaphoreType.DMA((4, n_zero)),
            pltpu.SemaphoreType.DMA,
            pltpu.SemaphoreType.DMA((2, len(pieces))),
            pltpu.SemaphoreType.DMA((2, n_zero, len(pieces))),
            pltpu.SemaphoreType.DMA((3, 2)),
        ],
        compiler_params=pltpu.CompilerParams(
            collective_id=0, has_side_effects=True, vmem_limit_bytes=60 * 2**20
        ),
        name="carry",
    )(*arrays, share, train, step)


def spread_kernel(n_model, part_ref, all_ref, sent, got, own):
    m = lax.axis_index("model")
    barrier = pltpu.get_barrier_semaphore()
    peers = [lax.rem(m + k, n_model) for k in range(1, n_model)]
    for peer in peers:
        pl.semaphore_signal(barrier, inc=1, device_id={"model": peer}, device_id_type=MESH)
    mine = pltpu.make_async_copy(part_ref, all_ref.at[m], own)
    mine.start()
    pl.semaphore_wait(barrier, n_model - 1)
    copies = []
    for k, peer in enumerate(peers, 1):
        copies.append(
            pltpu.make_async_remote_copy(
                src_ref=part_ref,
                dst_ref=all_ref.at[m],
                send_sem=sent.at[k],
                recv_sem=got.at[k],
                device_id={"model": peer},
                device_id_type=MESH,
            )
        )
    for copy in copies:
        copy.start()
    for copy in copies + [mine]:
        copy.wait()


def spread(n_model, part):
    vmem = pl.BlockSpec(memory_space=pltpu.VMEM)
    return pl.pallas_call(
        functools.partial(spread_kernel, n_model),
        out_shape=jax.ShapeDtypeStruct((n_model,) + part.shape, part.dtype),
        in_specs=[vmem],
        out_specs=vmem,
        scratch_shapes=[
            pltpu.SemaphoreType.DMA((n_model,)),
            pltpu.SemaphoreType.DMA((n_model,)),
            pltpu.SemaphoreType.DMA,
        ],
        compiler_params=pltpu.CompilerParams(collective_id=1, has_side_effects=True),
        cost_estimate=pl.CostEstimate(flops=20_000_000, bytes_accessed=65536, transcendentals=0),
        name="spread",
    )(part)


def settle_kernel(plan, *refs):
    sources, targets, spaces = refs[0:3], refs[3:6], refs[6:9]
    read_sem, write_sem = refs[9:]

    def reading(i):
        which, low, count, slot, _ = plan[i]
        return pltpu.make_async_copy(sources[which].at[pl.ds(low, count)], spaces[which].at[slot], read_sem.at[i])

    def writing(i):
        which, low, count, slot, _ = plan[i]
        return pltpu.make_async_copy(spaces[which].at[slot], targets[which].at[pl.ds(low, count)], write_sem.at[i])

    def read_after(i):
        for k, step in enumerate(plan):
            if step[4] == i:
                reading(k).start()

    read_after(None)
    for i in range(len(plan)):
        reading(i).wait()
        writing(i).start()
        if i >= LAG:
            writing(i - LAG).wait()
            read_after(i - LAG)
    for i in range(max(0, len(plan) - LAG), len(plan)):
        writing(i).wait()


def settle(arrays):
    plan, spaces = [], []
    for which in (1, 2, 0):
        step = arrays[which].shape[0] // COPIES[which]
        first = len(plan)
        for k in range(COPIES[which]):
            after = first + k - SLOTS[which] if k >= SLOTS[which] else None
            plan.append((which, k * step, step, k % SLOTS[which], after))
    for which, array in enumerate(arrays):
        step = array.shape[0] // COPIES[which]
        spaces.append(pltpu.VMEM((SLOTS[which], step, array.shape[1]), array.dtype))
    hbm = pl.BlockSpec(memory_space=pl.ANY)
    size = sum(array.shape[0] * array.shape[1] for array in arrays)
    return pl.pallas_call(
        functools.partial(settle_kernel, tuple(plan)),
        out_shape=tuple(jax.ShapeDtypeStruct(array.shape, array.dtype) for array in arrays),
        in_specs=[hbm] * 3,
        out_specs=(hbm,) * 3,
        scratch_shapes=spaces
        + [pltpu.SemaphoreType.DMA((len(plan),)), pltpu.SemaphoreType.DMA((len(plan),))],
        compiler_params=pltpu.CompilerParams(vmem_limit_bytes=40 * 2**20),
        cost_estimate=pl.CostEstimate(flops=8 * size, bytes_accessed=4 * size, transcendentals=0),
        name="settle",
    )(*arrays)


def on_device(n_zero, n_model, *args):
    arrays = args[:6]
    mix_share, norm_train, norm_step = args[6:]
    rows = mix_share.shape[0]
    z, unit = lax.axis_index("zero"), lax.axis_index("unit")
    edges = (0, 3 * rows // 32, rows // 4, rows)
    pieces = [(1, low, high - low, late) for low, high, late in zip(edges, edges[1:], (RAW, 0, 0))]
    pieces.append((2, 0, rows, 0))
    bounds = [cut * rows // CUTS[-1] for cut in CUTS]
    for k, late in enumerate(LATES):
        pieces.append((0, bounds[k], bounds[k + 1] - bounds[k], late))
    results = carry(
        n_zero,
        tuple(pieces),
        arrays,
        mix_share.reshape(-1, LANES),
        norm_train[None, :],
        norm_step[None, :],
    )
    serve, totals, gain, lates = list(results[:3]), results[3:6], results[6], results[7:]
    swap = [(k, k ^ 1) for k in range(n_zero)]
    partner = z + 1 - 2 * lax.rem(z, 2)
    landed = serve[0]
    serve = list(settle(serve))
    for late in range(1, LATE + 1):
        _, low, count, _ = pieces[LATES.index(late) - len(LATES)]
        where = (partner * rows + low, jnp.zeros_like(z))
        if late != STAGGER:
            block = lax.ppermute(lates[late - 1], "zero", swap)
        else:
            block = lax.ppermute(lates[late - 1], ("unit", "zero"), swap)
            there = lax.dynamic_slice(landed, where, (count, landed.shape[1]))
            block = jnp.where(unit == 0, block, there)
        serve[0] = lax.dynamic_update_slice(serve[0], block, where)
    totals, gain, _ = lax.optimization_barrier((totals, gain, serve[1]))
    factors = [jnp.sqrt(total[0]) for total in totals]
    gain = spread(n_model, gain)
    gain = gain.reshape(n_model, n_zero, -1).transpose(1, 0, 2)
    return (*serve, *factors, gain.reshape(-1))


def solution(mesh):
    in_specs = (
        P(("unit", "zero"), "model"),
        P(("unit", "zero"), "model"),
        P(("unit", "zero"), "model"),
        P(("unit", "zero"), "model"),
        P(("unit", "zero"), "model"),
        P(("unit", "zero"), "model"),
        P(("unit", "zero")),
        P(("unit", "zero", "model")),
        P(("unit", "zero", "model")),
    )
    out_specs = (
        P("unit", "model"),
        P("unit", "model"),
        P("unit", "model"),
        P(("unit", "model")),
        P(("unit", "model")),
        P(("unit", "model")),
        P("unit"),
    )
    return jax.shard_map(
        functools.partial(on_device, mesh.shape["zero"], mesh.shape["model"]),
        mesh=mesh,
        in_specs=in_specs,
        out_specs=out_specs,
        check_vma=False,
    )
```
